128 devices in a mesh: seq: 8 (over y_lo, x), exp: 16 (over y_hi, z, core).
Axes of the slice: x: 4, y: 4 (y_hi: 2, y_lo: 2; y = y_hi * 2 + y_lo), z: 4, core: 2. Of those that a mesh axis runs over, the one named last changes fastest.
Arguments:
- gates: float32 [16384, 2], P(('seq', 'exp')), may hold values from 0.1 to 0.9
- expert_ids: int32 [16384, 2], P(('seq', 'exp')), may hold values from 0 to 15, all different within a row; in each aligned block of 128 rows (0 to 127, 128 to 255, ...) at most 16 rows name the same one
- saved_pre: bfloat16 [16, 2048, 2, 7168], P('exp', None, None, 'seq'), may hold values from -6 to 6
- w_down: bfloat16 [16, 7168, 4096], P('exp', 'seq'), may hold values from -0.0625 to 0.0625
- residual_grad: bfloat16 [16384, 4096], P(('seq', 'exp')), may hold values from -6 to 6
- in_weight: bfloat16 [4096, 4096], P('seq', 'exp'), may hold values from -0.09375 to 0.09375
- ssm_in: bfloat16 [16384, 4096], P('seq', 'exp'), may hold values from -0.59765625 to 0.59765625
- b_proj: bfloat16 [16384, 128], P('seq'), may hold values from -0.546875 to 0.546875
- c_proj: bfloat16 [16384, 128], P('seq'), may hold values from -0.546875 to 0.546875
- step_sizes: float32 [64, 16384], P('exp', 'seq'), may hold values from 0.05 to 4590.52
- a_log: float32 [64], P('exp'), may hold values from -12 to 0
- skip_gain: float32 [64], P('exp'), may hold values from 0.5 to 1.5
- ssm_grad: bfloat16 [16384, 4096], P('seq', 'exp'), may hold values from -6 to 6
Outputs:
- pre_grads: bfloat16 [16, 2048, 2, 7168], P('exp', None, None, 'seq')
- route_grads: float32 [16384, 2], P(('seq', 'exp'))
- b_grads: float32 [16384, 128], P(('seq', 'exp'))
- c_grads: float32 [16384, 128], P(('seq', 'exp'))
- step_grads: float32 [64, 16384], P('exp', 'seq')
The draws below stay inside these ranges and needn't reach their ends.
Inputs may be any that keep to these rules, and one draw needn't show every extreme that they name: `expert_ids`: in each aligned block of 128 rows every expert is named by exactly 16 entries, and a row names 2 different experts.
All inputs are finite; a program needn't handle non-finite values.
Results may differ from the reference program's by a relative error of at most 0.019.
Values may be sent and summed in bfloat16 or wider, within the bound.
A program may use at most 192 MiB of HBM per device.

```python
import math
import jax
import jax.numpy as jnp
import numpy as np
from jax import lax

D = 4096
FFW = 7168
EXPERTS = 16
TOPK = 2
TOK_DEV = 128
TIME_HORIZON = 16384
TOKENS = 16384
CAP = 16
ESLOTS = 2048
HEAD_DEV = 4
CHANNEL_GROUPS = 64
HDIM = 64
NSTATE = 128
SPAN = 256
N_SEQ = 8
N_EXP = 16


def rate_fields(key):
    sampler_seeds = jax.random.split(jax.random.fold_in(key, 11), 6)
    fast_share = 0.5
    fast_heads = jax.random.uniform(sampler_seeds[0], (CHANNEL_GROUPS,)) < fast_share
    fast_rate = jax.random.uniform(sampler_seeds[1], (CHANNEL_GROUPS,), minval=0.2, maxval=0.35)
    slow_rate = jnp.exp(jax.random.uniform(sampler_seeds[2], (CHANNEL_GROUPS,), minval=jnp.log(0.2), maxval=jnp.log(0.6))) / (0.11 * TIME_HORIZON)
    forgetting_multiplier = jnp.where(fast_heads, fast_rate, slow_rate)
    drawn_increments = jnp.exp(jax.random.uniform(sampler_seeds[3], (CHANNEL_GROUPS, TIME_HORIZON), minval=jnp.log(0.05), maxval=jnp.log(0.2)))
    surge_instant = jax.random.randint(sampler_seeds[4], (3,), 0, TIME_HORIZON)
    surge_indicator = jnp.any(jnp.arange(TIME_HORIZON)[None, :] == surge_instant[:, None], axis=0)
    surge_magnitude = jax.random.uniform(sampler_seeds[5], (CHANNEL_GROUPS, TIME_HORIZON), minval=0.22, maxval=0.5)
    increment_elements = jnp.where(surge_indicator[None, :], surge_magnitude / forgetting_multiplier[:, None], drawn_increments)
    return (jnp.log(forgetting_multiplier).astype(jnp.float32), increment_elements.astype(jnp.float32))


def draw_a_log(key, part):
    return rate_fields(key)[0]


def draw_step_sizes(key, part):
    return rate_fields(key)[1]


def block_scale(rng, shape, shards, smallest, top_value):
    gain, own = 1.0, jax.random.fold_in(rng, 6)
    for axis_at, shards_of in shards:
        draws = jnp.exp(jax.random.uniform(jax.random.fold_in(own, axis_at), (shards_of,), jnp.float32, smallest / len(shards), top_value / len(shards)))
        gain = gain * jnp.repeat(draws, shape[axis_at] // shards_of).reshape([-1 if axis == axis_at else 1 for axis in range(len(shape))])
    return gain


def deal_out(key, own, number, rows, count, top, bound, skew):
    order = jax.random.permutation(key, count)
    heavy_load, common = shares(count, rows * top, bound, skew, True), shares(count, rows * top, bound, skew, False)
    places = jnp.arange(count)

    def named(tallies, rotation):
        used = int((tallies > 0).sum())
        fixed = max(1, used // 4)
        shifted = fixed + (places - fixed + rotation * (used - fixed)) % max(1, count - fixed)
        return jnp.zeros((count,), jnp.int32).at[order[jnp.where(places < fixed, places, shifted)]].set(jnp.asarray(tallies, jnp.int32))

    tallies = jnp.where(number % 4 == 0, named(heavy_load, number // 4), named(common, number - number // 4 - 1))
    mixed = jax.random.permutation(jax.random.fold_in(own, 3), count)
    source_of, sink = mixed[0:count // 2 * 2:2], mixed[1:count // 2 * 2:2]
    room = jnp.minimum(tallies[source_of] - 1, bound - tallies[sink]) // 2
    room = jnp.where((source_of == order[0]) | (sink == order[0]) | (tallies[sink] == 0), 0, jnp.maximum(room, 0))
    shifted = jax.random.randint(jax.random.fold_in(own, 4), (count // 2,), 0, 1 << 20) % (room + 1)
    tallies = tallies.at[source_of].add(-shifted).at[sink].add(shifted)
    items = jnp.searchsorted(jnp.cumsum(tallies), jnp.arange(rows * top), side="right").astype(jnp.int32)
    table = items.reshape(top, rows).T
    table = table[jax.random.permutation(jax.random.fold_in(own, 1), rows)]
    rotation = jax.random.randint(jax.random.fold_in(own, 2), (rows, 1), 0, top)
    return jnp.take_along_axis(table, (jnp.arange(top)[None, :] + rotation) % top, axis=1)


def shares(number_of, total, bound, lean, full):
    weights = [(1 << 20) // math.isqrt(standing ** lean) + 1 for standing in range(1, number_of + 1)]
    largest = bound if full else min(bound, max(-(-total // number_of), total * weights[0] // sum(weights)))
    least = 1 if total - largest >= number_of - 1 else 0
    counts, spare = [largest] + [least] * (number_of - 1), total - largest - least * (number_of - 1)
    while spare > 0:
        free = [i for i in range(1, number_of) if counts[i] < largest] or [i for i in range(1, number_of) if counts[i] < bound]
        whole, remaining = sum([weights[i] for i in free]), spare
        for i in free:
            addition = min(bound - counts[i], max(1, remaining * weights[i] // whole), spare)
            counts[i] = counts[i] + addition
            spare = spare - addition
    return np.array(counts)


def gaussian(stream_key, shape, scale, reach, cuts=(), kind=jnp.bfloat16):
    values = scale * jax.random.normal(stream_key, shape, jnp.float32)
    if cuts:
        values = values * block_scale(stream_key, shape, cuts, -0.22, 0.18)
    return jnp.clip(values, -reach, reach).astype(kind)


def setup_inputs(seed: int = 0) -> dict:
    seeds = jax.random.split(jax.random.key(seed), 14)
    gates = jnp.clip(0.1 + 0.79999997 * jax.random.uniform(seeds[0], (TOKENS, TOPK), jnp.float32) ** block_scale(seeds[0], (TOKENS, TOPK), ((0, 128),), -0.2, 0.2), 0.1, 0.9)
    expert_ids_keys = jax.random.split(jax.random.fold_in(seeds[1], 1), TOKENS // TOK_DEV)
    expert_ids_turns = jax.random.permutation(jax.random.fold_in(seeds[1], 3), TOKENS // TOK_DEV)
    expert_ids = jax.vmap(lambda own, number: deal_out(jax.random.fold_in(seeds[1], 2), own, number, TOK_DEV, EXPERTS, TOPK, CAP, 0))(expert_ids_keys, expert_ids_turns).reshape((TOKENS, TOPK))
    saved_pre = gaussian(seeds[2], (EXPERTS, ESLOTS, 2, FFW), 1.0, 6.0, ((0, 16), (3, 8)))
    w_down = gaussian(seeds[3], (EXPERTS, FFW, D), FFW ** -0.5, 0.0625, ((0, 16), (1, 8)))
    residual_grad = gaussian(seeds[4], (TOKENS, D), 1.0, 6.0, ((0, 128),))
    in_weight = gaussian(seeds[5], (D, CHANNEL_GROUPS * HDIM), (CHANNEL_GROUPS * HDIM) ** -0.5, 0.09375, ((0, 8), (1, 16)))
    ssm_in = gaussian(seeds[6], (TIME_HORIZON, CHANNEL_GROUPS * HDIM), 0.1, 0.59765625, ((0, 8), (1, 16)))
    b_proj = gaussian(seeds[7], (TIME_HORIZON, NSTATE), 0.088, 0.546875, ((0, 8),))
    c_proj = gaussian(seeds[8], (TIME_HORIZON, NSTATE), 0.088, 0.546875, ((0, 8),))
    step_sizes = draw_step_sizes(jax.random.fold_in(seeds[13], 71), 0)
    a_log = draw_a_log(jax.random.fold_in(seeds[13], 71), 0)
    skip_gain = jnp.clip(0.5 + 1.0 * jax.random.uniform(seeds[11], (CHANNEL_GROUPS,), jnp.float32) ** block_scale(seeds[11], (CHANNEL_GROUPS,), ((0, 16),), -0.2, 0.2), 0.5, 1.5)
    ssm_grad = gaussian(seeds[12], (TIME_HORIZON, CHANNEL_GROUPS * HDIM), 1.0, 6.0, ((0, 8), (1, 16)))
    return dict(gates=gates, expert_ids=expert_ids, saved_pre=saved_pre, w_down=w_down, residual_grad=residual_grad, in_weight=in_weight, ssm_in=ssm_in, b_proj=b_proj, c_proj=c_proj, step_sizes=step_sizes, a_log=a_log, skip_gain=skip_gain, ssm_grad=ssm_grad)


PRECISE = lax.Precision.HIGHEST

def span_scan(heads_input, b_values, c_values, log_decay, skip_values, start_state):
    head_count, length, head_size = heads_input.shape
    state_size = b_values.shape[1]
    blocks = length // SPAN
    x_spans = heads_input.reshape(head_count, blocks, SPAN, head_size).transpose(1, 0, 2, 3)
    b_spans = b_values.reshape(blocks, SPAN, state_size)
    c_spans = c_values.reshape(blocks, SPAN, state_size)
    g_spans = log_decay.reshape(head_count, blocks, SPAN).transpose(1, 0, 2)
    lower_mask = jnp.tril(jnp.ones((SPAN, SPAN), jnp.bool_))

    def advance(carried_state, inputs):
        x_block, b_block, c_block, g_block = inputs
        cumulative = jnp.cumsum(g_block, axis=1)
        spread = cumulative[:, :, None] - cumulative[:, None, :]
        weights = jnp.where(lower_mask, jnp.exp(-jnp.where(lower_mask, spread, 0.0)), 0.0)
        scores = jnp.dot(c_block, b_block.T, precision=PRECISE)
        within = jnp.einsum('hij,ij,hjp->hip', weights, scores, x_block, precision=PRECISE)
        carried = jnp.einsum('hi,in,hpn->hip', jnp.exp(-cumulative), c_block, carried_state, precision=PRECISE)
        tail_decay = jnp.exp(cumulative - cumulative[:, -1:])
        fresh_state = jnp.einsum('hj,hjp,jn->hpn', tail_decay, x_block, b_block, precision=PRECISE)
        next_state = jnp.exp(-cumulative[:, -1])[:, None, None] * carried_state + fresh_state
        return (next_state, within + carried)
    final_state, outputs = lax.scan(advance, start_state, (x_spans, b_spans, c_spans, g_spans))
    output = outputs.transpose(1, 0, 2, 3).reshape(head_count, length, head_size)
    return (output + skip_values[:, None, None] * heads_input, final_state)

def swiglu_grads(upstream, gate_values, saved_rows):
    gate_pre = saved_rows[:, 0, :].astype(jnp.float32)
    up_pre = saved_rows[:, 1, :].astype(jnp.float32)
    sigmoid_gate = jax.nn.sigmoid(gate_pre)
    activated = gate_pre * sigmoid_gate
    route_part = lax.optimization_barrier(jnp.sum(activated * up_pre * upstream, axis=1))
    hidden_grad = gate_values[:, None] * upstream
    gate_grad = hidden_grad * up_pre * sigmoid_gate * (1.0 + gate_pre * (1.0 - sigmoid_gate))
    up_grad = hidden_grad * activated
    return (jnp.stack([gate_grad, up_grad], axis=1).astype(jnp.bfloat16), route_part)

def reference(gates, expert_ids, saved_pre, w_down, residual_grad, in_weight, ssm_in, b_proj, c_proj, step_sizes, a_log, skip_gain, ssm_grad):
    heads_input = ssm_in.astype(jnp.float32).reshape(TIME_HORIZON, CHANNEL_GROUPS, HDIM).transpose(1, 0, 2)
    grads_heads = ssm_grad.astype(jnp.float32).reshape(TIME_HORIZON, CHANNEL_GROUPS, HDIM).transpose(1, 0, 2)
    decay_rates = jnp.exp(a_log)

    def forward(inputs, b_values, c_values, sizes):
        outputs, unused = span_scan(inputs, b_values, c_values, sizes * decay_rates[:, None], skip_gain, jnp.zeros((CHANNEL_GROUPS, HDIM, NSTATE), jnp.float32))
        return outputs
    unused, pullback = jax.vjp(forward, heads_input, b_proj.astype(jnp.float32), c_proj.astype(jnp.float32), step_sizes)
    input_heads, b_grads, c_grads, step_grads = pullback(grads_heads)
    x_grad = input_heads.transpose(1, 0, 2).reshape(TIME_HORIZON, CHANNEL_GROUPS * HDIM).astype(jnp.bfloat16)
    group_width = HEAD_DEV * HDIM
    grad_groups = x_grad.reshape(TIME_HORIZON, N_EXP, group_width).transpose(1, 0, 2)
    weight_groups = in_weight.reshape(D, N_EXP, group_width).transpose(1, 0, 2)

    def add_group(total, pair):
        head_part = jnp.dot(pair[0], pair[1].T, preferred_element_type=jnp.float32).astype(jnp.bfloat16)
        head_part = lax.optimization_barrier(head_part).astype(jnp.float32)
        return (total + head_part, None)
    summed, unused_out = lax.scan(add_group, residual_grad.astype(jnp.float32), (grad_groups, weight_groups))
    moe_grad = summed.astype(jnp.bfloat16)
    device_count = N_SEQ * N_EXP
    per_block = expert_ids.reshape(device_count, TOK_DEV * TOPK)
    onehot = (per_block[:, :, None] == jnp.arange(EXPERTS, dtype=jnp.int32)[None, None, :]).astype(jnp.int32)
    running = jnp.cumsum(onehot, axis=1)
    position = lax.optimization_barrier(jnp.sum(onehot * running, axis=2)) - 1
    slot_row = (jnp.arange(device_count, dtype=jnp.int32)[:, None] * CAP + position).reshape(-1).astype(jnp.int32)
    expert_flat = per_block.reshape(-1).astype(jnp.int32)
    assignment = jnp.arange(TOKENS * TOPK, dtype=jnp.int32)
    table = jnp.zeros((EXPERTS, ESLOTS), jnp.int32).at[expert_flat, slot_row].set(assignment)
    gate_flat = gates.reshape(-1)

    def one_expert(expert_index):
        members = table[expert_index]
        row_block = moe_grad[members // TOPK]
        upstream = jnp.dot(row_block, w_down[expert_index].T, preferred_element_type=jnp.float32)
        return swiglu_grads(upstream, gate_flat[members], saved_pre[expert_index])
    pre_grads, route_slots = lax.map(one_expert, jnp.arange(EXPERTS, dtype=jnp.int32))
    route_grads = route_slots[expert_flat, slot_row].reshape(TOKENS, TOPK)
    return (pre_grads, route_grads, b_grads, c_grads, step_grads)
```

```python
import functools

import jax
import jax.numpy as jnp
from jax import lax
from jax.experimental import pallas as pl
from jax.experimental.pallas import tpu as pltpu
from jax.sharding import Mesh
from jax.sharding import PartitionSpec as P

TOPK = 2
HDIM = 64
SPAN = 256
CHIPS = ("exp_0", "exp_1")
CORE = "exp_2"
EXP = ("exp_0", "exp_1", "exp_2")
SEQ_EXP = ("seq", "exp_0", "exp_1", "exp_2")
F32 = jnp.float32
BF16 = jnp.bfloat16
MESH = pl.DeviceIdType.MESH


def nn(a, b):
    return lax.dot_general(a, b, (((1,), (0,)), ((), ())), preferred_element_type=F32)


def nt(a, b):
    return lax.dot_general(a, b, (((1,), (1,)), ((), ())), preferred_element_type=F32)


def tn(a, b):
    return lax.dot_general(a, b, (((0,), (0,)), ((), ())), preferred_element_type=F32)


def over_lanes(columns):
    rows, heads = columns.shape
    lane = lax.broadcasted_iota(jnp.int32, (rows, 2 * HDIM), 1)
    return jnp.concatenate(
        [
            jnp.where(lane < HDIM, columns[:, h : h + 1], columns[:, h + 1 : h + 2])
            for h in range(0, heads, 2)
        ],
        axis=1,
    )


def decays(lcol_ref):
    running = lcol_ref[...]
    last = running[SPAN - 1 : SPAN, :]
    return over_lanes(jnp.exp(-running)), over_lanes(jnp.exp(running - last))


def barrier_with(peers):
    semaphore = pltpu.get_barrier_semaphore()
    for peer in peers:
        pl.semaphore_signal(semaphore, inc=1, device_id=peer, device_id_type=MESH)
    pl.semaphore_wait(semaphore, len(peers))


ORDERS = ("xyz", "yzx", "zxy", "xzy", "yxz", "zyx")
UNIT = 16


class Torus:
    def __init__(self):
        seq = lax.axis_index("seq")
        self.at = {
            "x": lax.rem(seq, 4),
            "y": lax.axis_index("exp_0") * 2 + lax.div(seq, 4),
            "z": lax.axis_index("exp_1"),
        }

    def device(self, dim, step):
        at = dict(self.at)
        at[dim] = lax.rem(at[dim] + (step + 4), 4)
        return {"seq": lax.rem(at["y"], 2) * 4 + at["x"], "exp_0": lax.div(at["y"], 2), "exp_1": at["z"]}


class Gather:
    def __init__(self, torus, own_ref, out_ref, send_sem, recv_sem):
        self.torus, self.own, self.out = torus, own_ref, out_ref
        self.send_sem, self.recv_sem = send_sem, recv_sem
        units = own_ref.shape[0] // UNIT
        count = len(ORDERS)
        ends = [units * k // count * UNIT for k in range(count + 1)]
        self.rows = [(ends[k], ends[k + 1] - ends[k]) for k in range(count)]

    def block(self, stream, phase, step, start, size):
        order = ORDERS[stream]
        at = []
        for dim in "xyz":
            k = order.index(dim)
            if k < phase:
                at.append(slice(None))
            elif k == phase:
                at.append(lax.rem(self.torus.at[dim] + (step + 4), 4))
            else:
                at.append(self.torus.at[dim])
        return self.out.at[(*at, pl.ds(start, size), slice(None))]

    def copies(self, stream, step, back=False):
        phase, second = step // 2, step % 2
        dim = ORDERS[stream][phase]
        start, size = self.rows[stream]
        half = (size // UNIT + 1) // 2 * UNIT
        made = []
        for side, way in enumerate((1, -1)):
            if not second:
                span, hop = (start, size), 0
            else:
                span = (start, half) if side == 0 else (start + half, size - half)
                hop = -way
            sent = self.block(stream, phase, hop, *span)
            here = sent
            if step == 0:
                sent = self.own.at[pl.ds(*span), :]
            common = dict(
                send_sem=self.send_sem.at[stream, step, side],
                recv_sem=self.recv_sem.at[stream, step, side],
                device_id=self.torus.device(dim, way),
                device_id_type=MESH,
            )
            if back:
                sent = here = self.block(stream, phase, hop - way, *span)
            made.append(pltpu.make_async_remote_copy(src_ref=sent, dst_ref=here, **common))
        return made

    def start(self, stream, step):
        for copy in self.copies(stream, step):
            copy.start()

    def arrived(self, stream, step):
        for copy in self.copies(stream, step, back=True):
            copy.wait_recv()

    def advance(self, step, streams):
        for stream in streams:
            if step > 0:
                self.arrived(stream, step - 1)
            if step < 6:
                self.start(stream, step)

    def drain(self):
        for stream in range(len(ORDERS)):
            for step in range(6):
                for copy in self.copies(stream, step):
                    copy.wait_send()


def ssm_kernel(
    w_ref, x_ref, g_ref, b_ref, c_ref, lcol_ref, lrow_ref, whole_ref, before_ref, tail_ref, skip_ref, rate_ref,
    all_ref, dx_ref, dbc_ref, dq_ref,
    s_all, g_all, s_acc, g_acc, ends, got, dx_all,
    own_sem, w_send, w_recv, s_send, s_recv, x_send, x_recv,
):
    chunks = s_all.shape[0]
    parts = got.shape[0]
    width = x_ref.shape[1]
    heads = width // HDIM
    torus = Torus()
    me = lax.axis_index("seq")
    place = lax.axis_index("exp_0") * 4 + lax.axis_index("exp_1")

    def in_part(offset):
        return lax.rem(me + offset, parts)

    def chip_at(index):
        return {"exp_0": lax.div(index, 4), "exp_1": lax.rem(index, 4)}

    across_y = {"seq": lax.rem(me + 4, 8), "exp_0": 1 - lax.axis_index("exp_0")}
    barrier_with(
        [{"seq": in_part(o)} for o in range(1, parts)]
        + [chip_at(lax.rem(place + o, chunks)) for o in range(1, chunks)]
        + [across_y]
    )
    gather = Gather(torus, w_ref, all_ref, w_send, w_recv)
    streams = range(len(ORDERS))
    gather.advance(0, streams)
    here = torus.at
    own = pltpu.make_async_copy(w_ref, all_ref.at[here["x"], here["y"], here["z"]], own_sem.at[0])
    own.start()

    def rows_of(chunk):
        return pl.ds(pl.multiple_of(chunk * SPAN, SPAN), SPAN)

    s_acc[...] = jnp.zeros_like(s_acc)
    g_acc[...] = jnp.zeros_like(g_acc)

    def states(chunk, carry):
        rows = rows_of(chunk)
        from_start, to_end = decays(lcol_ref.at[rows])
        fresh = tn(b_ref[rows, :], (x_ref[rows, :].astype(F32) * to_end).astype(BF16))
        back = tn(c_ref[rows, :], (g_ref[rows, :].astype(F32) * from_start).astype(BF16))
        s_all[chunk] = fresh
        g_all[chunk] = back
        s_acc[...] = s_acc[...] * whole_ref[chunk] + fresh
        g_acc[...] = g_acc[...] + before_ref[chunk] * back
        return carry

    lax.fori_loop(0, chunks, states, 0)
    ends[0, :128, :] = s_acc[...].astype(BF16)
    ends[1, :128, :] = g_acc[...].astype(BF16)
    ends[0, 128:, :] = tail_ref[...]
    ends[1, 128:, :] = tail_ref[...]

    def to_part(offset, back=False):
        peer = in_part(offset)
        source = in_part(parts - offset)
        common = dict(
            send_sem=s_send.at[offset - 1], recv_sem=s_recv.at[offset - 1], device_id={"seq": peer}, device_id_type=MESH
        )
        which = jnp.where(peer > me, 0, 1)
        if back:
            return pltpu.make_async_remote_copy(src_ref=got.at[source], dst_ref=got.at[source], **common)
        return pltpu.make_async_remote_copy(src_ref=ends.at[which], dst_ref=got.at[me], **common)

    for offset in range(1, parts):
        to_part(offset).start()
    own.wait()
    gather.advance(1, streams)
    got[me] = jnp.zeros(got.shape[1:], BF16)
    for offset in range(1, parts):
        to_part(offset, back=True).wait_recv()
    gather.advance(2, streams)

    def decay_of(m):
        return got[m, 128:129, :].astype(F32) + got[m, 129:130, :].astype(F32)

    state = jnp.zeros((128, width), F32)
    for m in range(parts):
        state = jnp.where(m < me, decay_of(m) * state + got[m, :128, :].astype(F32), state)
    for k in range(chunks):
        fresh = s_all[k]
        s_all[k] = state
        state = state * whole_ref[k] + fresh
    state = jnp.zeros((128, width), F32)
    for m in reversed(range(parts)):
        state = jnp.where(m > me, decay_of(m) * state + got[m, :128, :].astype(F32), state)
    for k in reversed(range(chunks)):
        fresh = g_all[k]
        g_all[k] = state
        state = state * whole_ref[k] + fresh

    row = lax.broadcasted_iota(jnp.int32, (SPAN, SPAN), 0)
    col = lax.broadcasted_iota(jnp.int32, (SPAN, SPAN), 1)
    head_of = lax.broadcasted_iota(jnp.int32, (8, width), 1) // HDIM
    pick = (head_of == lax.broadcasted_iota(jnp.int32, (8, width), 0)).astype(F32)
    pick_half = pick.astype(BF16)

    def to_chip(turn, back=False):
        target = lax.rem(place + 1 + turn, chunks)
        source = lax.rem(place + (chunks - 1) - turn, chunks)
        common = dict(
            send_sem=x_send.at[turn], recv_sem=x_recv.at[turn], device_id=chip_at(target), device_id_type=MESH
        )
        if back:
            return pltpu.make_async_remote_copy(src_ref=dx_ref.at[source], dst_ref=dx_ref.at[source], **common)
        return pltpu.make_async_remote_copy(src_ref=dx_all.at[target], dst_ref=dx_ref.at[place], **common)

    def grads(turn, carry):
        chunk = lax.rem(place + 1 + turn, chunks)
        rows = rows_of(chunk)
        x = x_ref[rows, :]
        g = g_ref[rows, :]
        b = b_ref[rows, :]
        c = c_ref[rows, :]
        lcol = lcol_ref[rows, :]
        lrow = lrow_ref[:, rows]
        s_in = s_all[chunk]
        g_out = g_all[chunk]
        s_half = s_in.astype(BF16)
        g_half = g_out.astype(BF16)
        upper = row <= col
        strict = row < col
        from_row = (row >= col).astype(F32).astype(BF16)
        before_row = strict.astype(F32).astype(BF16)
        bc = nt(b, c)
        dx = jnp.zeros((SPAN, width), F32)
        pairs = jnp.zeros((SPAN, SPAN), F32)
        inside = []
        for h in range(heads):
            mine = pick_half[h : h + 1, :]
            m = nt(x * mine, g)
            w = jnp.exp(jnp.where(upper, lcol[:, h : h + 1] - lrow[h : h + 1, :], -1e30))
            a1 = w * bc
            pairs = pairs + w * m
            dx = dx + nn(a1.astype(BF16), g * mine)
            p = jnp.where(strict, a1 * m, 0.0).astype(BF16)
            inside.append(jnp.sum(jnp.where(strict, nn(p, from_row), 0.0), axis=0, keepdims=True))
        from_start, to_end = decays(lcol_ref.at[rows])
        ge = (g.astype(F32) * from_start).astype(BF16)
        xe = (x.astype(F32) * to_end).astype(BF16)
        pairs_half = pairs.astype(BF16)
        z = nn(c, s_half)
        v = nn(b, g_half)
        dbc_ref[rows, :128] = nn(pairs_half, c) + nt(xe, g_half)
        dbc_ref[rows, 128:] = tn(pairs_half, b) + nt(ge, s_half)
        dx_all[chunk] = (dx + to_end * v + skip_ref[...] * g.astype(F32)).astype(BF16)

        @pl.when(turn < chunks - 1)
        def _():
            to_chip(turn).start()

        rc = nt(pick_half, (ge.astype(F32) * z).astype(BF16))
        cc = nt(pick_half, (xe.astype(F32) * v).astype(BF16))
        across = jnp.sum(s_in * g_out, axis=0, keepdims=True) * whole_ref[chunk]
        ones = jnp.ones((width, SPAN), BF16)
        dq = nn(rc.astype(BF16), from_row) + nn(cc.astype(BF16), before_row) + nn((pick * across).astype(BF16), ones)
        for h in range(heads):
            dq_ref[h : h + 1, rows] = -(dq[h : h + 1, :] + inside[h]) * rate_ref[h : h + 1, :]
        for step, after in STEPS_AFTER:

            @pl.when(turn == after)
            def _(step=step):
                gather.advance(step, streams)

        return carry

    lax.fori_loop(0, chunks, grads, 0)
    mine = pltpu.make_async_copy(dx_all.at[place], dx_ref.at[place], own_sem.at[0])
    mine.start()
    for step in LAST_STEPS:
        gather.advance(step, streams)
    mine.wait()
    for turn in range(chunks - 1):
        to_chip(turn, back=True).wait_recv()
        to_chip(turn).wait_send()
    for offset in range(1, parts):
        to_part(offset).wait_send()
    gather.drain()


STEPS_AFTER = ((3, 1), (4, 3))
LAST_STEPS = (5, 6)


def ssm_part(in_weight, ssm_in, b_proj, c_proj, step_sizes, a_log, skip_gain, ssm_grad):
    length, width = ssm_in.shape
    heads = width // HDIM
    chunks = length // SPAN
    parts = lax.axis_size("seq")
    rates = jnp.exp(a_log)
    steps = (step_sizes * rates[:, None]).reshape(heads * chunks, SPAN)
    at = jnp.arange(SPAN)
    lrow = jnp.dot(steps, (at[:, None] <= at[None, :]).astype(F32), precision=lax.Precision.HIGHEST)
    totals = lrow[:, -1].reshape(heads, chunks)
    lrow = lrow.reshape(heads, length)
    lcol = lrow.T
    whole = jnp.repeat(jnp.exp(-totals).T, HDIM, axis=1).reshape(chunks, 1, width)
    sums = jnp.cumsum(totals, axis=1)
    before = jnp.repeat(jnp.exp(-(sums - totals)).T, HDIM, axis=1).reshape(chunks, 1, width)
    device_decay = jnp.repeat(jnp.exp(-sums[:, -1]), HDIM)
    skip = jnp.repeat(skip_gain, HDIM).reshape(1, width)
    high = device_decay.astype(BF16)
    low = (device_decay - high.astype(F32)).astype(BF16)
    tail = jnp.pad(jnp.stack([high, low]), ((0, 14), (0, 0)))
    vmem = pl.BlockSpec(memory_space=pltpu.VMEM)
    hbm = pl.BlockSpec(memory_space=pl.ANY)
    streams = len(ORDERS)
    dma = pltpu.SemaphoreType.DMA
    return pl.pallas_call(
        ssm_kernel,
        out_shape=(
            jax.ShapeDtypeStruct((4, 4, 4, *in_weight.shape), BF16),
            jax.ShapeDtypeStruct((chunks, SPAN, width), BF16),
            jax.ShapeDtypeStruct((length, 256), F32),
            jax.ShapeDtypeStruct((heads, length), F32),
        ),
        in_specs=[vmem] * 12,
        out_specs=(hbm, hbm, vmem, vmem),
        scratch_shapes=[
            pltpu.VMEM((chunks, 128, width), F32),
            pltpu.VMEM((chunks, 128, width), F32),
            pltpu.VMEM((128, width), F32),
            pltpu.VMEM((128, width), F32),
            pltpu.VMEM((2, 144, width), BF16),
            pltpu.VMEM((parts, 144, width), BF16),
            pltpu.VMEM((chunks, SPAN, width), BF16),
            dma((1,)),
            dma((streams, 6, 2)),
            dma((streams, 6, 2)),
            dma((parts - 1,)),
            dma((parts - 1,)),
            dma((chunks - 1,)),
            dma((chunks - 1,)),
        ],
        compiler_params=pltpu.CompilerParams(
            collective_id=1, has_side_effects=True, vmem_limit_bytes=48 * 2**20
        ),
        name="ssm",
    )(in_weight, ssm_in, ssm_grad, b_proj, c_proj, lcol, lrow, whole, before, tail, skip, rates[:, None])


def project_kernel(core_ref, x_ref, w_ref, keep_ref, send_ref, total):
    core = core_ref[0]
    half = keep_ref.shape[0]
    width = x_ref.shape[2]
    acc = jnp.zeros(total.shape, F32)
    for k in range(x_ref.shape[0]):
        acc = acc + nt(x_ref[k], w_ref[0, k // 4, 0, k % 4])
    total[...] = acc
    keep_ref[...] = total[pl.ds(pl.multiple_of(core * half, half), half), :].astype(BF16)
    send_ref[...] = total[pl.ds(pl.multiple_of((1 - core) * half, half), half), :].astype(BF16)


def project(x_all, w_all):
    blocks, tokens, width = x_all.shape
    rows = w_all.shape[3]
    w_all = w_all.reshape(4, 2, 2, 4, rows, width)
    half = jax.ShapeDtypeStruct((tokens // 2, 8 * rows), BF16)
    return pl.pallas_call(
        project_kernel,
        grid=(8,),
        out_shape=(half, half),
        in_specs=[
            pl.BlockSpec(memory_space=pltpu.SMEM),
            pl.BlockSpec((blocks, tokens, width), lambda i: (0, 0, 0)),
            pl.BlockSpec((1, 2, 1, 4, rows, width), lambda i: (i % 4, 0, i // 4, 0, 0, 0)),
        ],
        out_specs=(pl.BlockSpec((tokens // 2, rows), lambda i: (0, i)),) * 2,
        scratch_shapes=[pltpu.VMEM((tokens, rows), F32)],
        compiler_params=pltpu.CompilerParams(dimension_semantics=("arbitrary",)),
        name="project",
    )(lax.axis_index(CORE).reshape(1).astype(jnp.int32), x_all, w_all)


def expert_kernel(a_ref, w_ref, saved_ref, pre_ref, route_ref):
    rows = a_ref.shape[0] * a_ref.shape[1]
    upstream = nt(a_ref[...].reshape(rows, a_ref.shape[2]), w_ref[0])
    gate_pre = saved_ref[:, 0, :].astype(F32)
    up_pre = saved_ref[:, 1, :].astype(F32)
    sig = jax.nn.sigmoid(gate_pre)
    act = gate_pre * sig
    up_grad = upstream * act
    gate_grad = upstream * up_pre * sig * (1.0 + gate_pre * (1.0 - sig))
    pre_ref[:, 0, :] = gate_grad.astype(BF16)
    pre_ref[:, 1, :] = up_grad.astype(BF16)
    route_ref[...] = nt(jnp.ones((8, up_pre.shape[1]), BF16), (up_grad * up_pre).astype(BF16))


def expert_part(gathered, w_down, saved_pre):
    parts, own, d = gathered.shape
    slots, _, hidden = saved_pre.shape[1:]
    step = 256
    per = step // own
    return pl.pallas_call(
        expert_kernel,
        grid=(slots // step,),
        out_shape=(
            jax.ShapeDtypeStruct((slots, 2, hidden), BF16),
            jax.ShapeDtypeStruct((8, slots), F32),
        ),
        in_specs=[
            pl.BlockSpec((per, own, d), lambda i: (i, 0, 0)),
            pl.BlockSpec((1, hidden, d), lambda i: (0, 0, 0)),
            pl.BlockSpec((step, 2, hidden), lambda i: (i, 0, 0)),
        ],
        out_specs=(
            pl.BlockSpec((step, 2, hidden), lambda i: (i, 0, 0)),
            pl.BlockSpec((8, step), lambda i: (0, i)),
        ),
        compiler_params=pltpu.CompilerParams(
            dimension_semantics=("arbitrary",), vmem_limit_bytes=60 * 2**20
        ),
        name="experts",
    )(gathered, w_down, saved_pre[0])


def per_device(
    gates, expert_ids, saved_pre, w_down, residual_grad, in_weight, ssm_in, b_proj, c_proj, step_sizes, a_log, skip_gain, ssm_grad
):
    w_all, x_all, bc_grads, step_grads = ssm_part(
        in_weight, ssm_in, b_proj, c_proj, step_sizes, a_log, skip_gain, ssm_grad
    )
    tokens_here, d = residual_grad.shape
    experts = lax.axis_size(EXP)
    parts = lax.axis_size("seq")
    capacity = TOPK * tokens_here // experts
    bc_grads = lax.psum_scatter(bc_grads, EXP, scatter_dimension=0, tiled=True)
    b_grads, c_grads = bc_grads[:, :128], bc_grads[:, 128:]
    keep, send = project(x_all, w_all)
    other = lax.ppermute(send, CORE, [(0, 1), (1, 0)])
    moe_grad = (residual_grad.astype(F32) + keep.astype(F32) + other.astype(F32)).astype(BF16)
    flat_ids = expert_ids.reshape(-1)
    onehot = (flat_ids[:, None] == jnp.arange(experts, dtype=jnp.int32)[None, :]).astype(jnp.int32)
    position = jnp.sum(onehot * jnp.cumsum(onehot, axis=0), axis=1) - 1
    target = flat_ids * capacity + position
    selector = target[:, None] == jnp.arange(experts * capacity, dtype=jnp.int32)[None, :]
    by_token = selector.reshape(tokens_here, TOPK, -1)
    slot_gates = jnp.sum(by_token * gates[:, :, None], axis=(0, 1))
    rows = tn(jnp.any(by_token, axis=1).astype(BF16), moe_grad)
    outgoing = (rows * slot_gates[:, None]).astype(BF16).reshape(experts, capacity, d)
    arrived = lax.all_to_all(outgoing, EXP, 0, 0, tiled=True).reshape(experts * capacity, d)
    gathered = lax.all_gather(arrived, "seq", axis=0, tiled=False)
    pre_grads, route = expert_part(gathered, w_down, saved_pre)
    route = route[0].reshape(parts * experts, capacity)
    route = lax.all_to_all(route, SEQ_EXP, 0, 0, tiled=True)
    totals = jnp.sum(route.reshape(parts, experts * capacity), axis=0)
    route_grads = totals[target].reshape(tokens_here, TOPK) / gates
    return (pre_grads[None], route_grads, b_grads, c_grads, step_grads)


def solution(mesh):
    split = Mesh(mesh.devices.reshape(mesh.shape["seq"], 2, 4, 2), ("seq", "exp_0", "exp_1", "exp_2"))
    in_specs = (
        P(SEQ_EXP, None), P(SEQ_EXP, None), P(EXP, None, None, "seq"), P(EXP, "seq", None), P(SEQ_EXP, None), P("seq", EXP),
        P("seq", EXP), P("seq", None), P("seq", None), P(EXP, "seq"), P(EXP), P(EXP), P("seq", EXP),
    )
    out_specs = (P(EXP, None, None, "seq"), P(SEQ_EXP, None), P(SEQ_EXP, None), P(SEQ_EXP, None), P(EXP, "seq"))
    return jax.shard_map(per_device, mesh=split, in_specs=in_specs, out_specs=out_specs, check_vma=False)
```

```python
import functools

import jax
import jax.numpy as jnp
from jax import lax
from jax.experimental import pallas as pl
from jax.experimental.pallas import tpu as pltpu
from jax.sharding import Mesh
from jax.sharding import PartitionSpec as P

TOPK = 2
HDIM = 64
SPAN = 256
CHIPS = ("exp_0", "exp_1")
CORE = "exp_2"
EXP = ("exp_0", "exp_1", "exp_2")
SEQ_EXP = ("seq", "exp_0", "exp_1", "exp_2")
F32 = jnp.float32
BF16 = jnp.bfloat16
MESH = pl.DeviceIdType.MESH


def nn(a, b):
    return lax.dot_general(a, b, (((1,), (0,)), ((), ())), preferred_element_type=F32)


def nt(a, b):
    return lax.dot_general(a, b, (((1,), (1,)), ((), ())), preferred_element_type=F32)


def tn(a, b):
    return lax.dot_general(a, b, (((0,), (0,)), ((), ())), preferred_element_type=F32)


def over_lanes(columns):
    rows, heads = columns.shape
    lane = lax.broadcasted_iota(jnp.int32, (rows, 2 * HDIM), 1)
    return jnp.concatenate(
        [
            jnp.where(lane < HDIM, columns[:, h : h + 1], columns[:, h + 1 : h + 2])
            for h in range(0, heads, 2)
        ],
        axis=1,
    )


def decays(lcol_ref):
    running = lcol_ref[...]
    last = running[SPAN - 1 : SPAN, :]
    return over_lanes(jnp.exp(-running)), over_lanes(jnp.exp(running - last))


def barrier_with(peers):
    semaphore = pltpu.get_barrier_semaphore()
    for peer in peers:
        pl.semaphore_signal(semaphore, inc=1, device_id=peer, device_id_type=MESH)
    pl.semaphore_wait(semaphore, len(peers))


ORDERS = ("xyz", "yzx", "zxy", "xzy", "yxz", "zyx")
SHARES = (5, 6, 5, 5, 5, 6)
UNIT = 16


class Torus:
    def __init__(self):
        seq = lax.axis_index("seq")
        self.at = {
            "x": lax.rem(seq, 4),
            "y": lax.axis_index("exp_0") * 2 + lax.div(seq, 4),
            "z": lax.axis_index("exp_1"),
        }

    def device(self, dim, step):
        at = dict(self.at)
        at[dim] = lax.rem(at[dim] + (step + 4), 4)
        return {"seq": lax.rem(at["y"], 2) * 4 + at["x"], "exp_0": lax.div(at["y"], 2), "exp_1": at["z"]}


class Gather:
    def __init__(self, torus, own_ref, out_ref, send_sem, recv_sem):
        self.torus, self.own, self.out = torus, own_ref, out_ref
        self.send_sem, self.recv_sem = send_sem, recv_sem
        self.rows = [(sum(SHARES[:k]) * UNIT, SHARES[k] * UNIT) for k in range(len(ORDERS))]

    def block(self, stream, phase, step, start, size):
        order = ORDERS[stream]
        at = []
        for dim in "xyz":
            k = order.index(dim)
            if k < phase:
                at.append(slice(None))
            elif k == phase:
                at.append(lax.rem(self.torus.at[dim] + (step + 4), 4))
            else:
                at.append(self.torus.at[dim])
        return self.out.at[(*at, pl.ds(start, size), slice(None))]

    def copies(self, stream, step, back=False):
        phase, second = step // 2, step % 2
        dim = ORDERS[stream][phase]
        start, size = self.rows[stream]
        half = (size // UNIT + 1) // 2 * UNIT
        made = []
        for side, way in enumerate((1, -1)):
            if not second:
                span, hop = (start, size), 0
            else:
                span = (start, half) if side == 0 else (start + half, size - half)
                hop = -way
            sent = self.block(stream, phase, hop, *span)
            here = sent
            if step == 0:
                sent = self.own.at[pl.ds(*span), :]
            common = dict(
                send_sem=self.send_sem.at[stream, step, side],
                recv_sem=self.recv_sem.at[stream, step, side],
                device_id=self.torus.device(dim, way),
                device_id_type=MESH,
            )
            if back:
                sent = here = self.block(stream, phase, hop - way, *span)
            made.append(pltpu.make_async_remote_copy(src_ref=sent, dst_ref=here, **common))
        return made

    def start(self, stream, step):
        for copy in self.copies(stream, step):
            copy.start()

    def arrived(self, stream, step):
        for copy in self.copies(stream, step, back=True):
            copy.wait_recv()

    def advance(self, step, streams):
        for stream in streams:
            if step > 0:
                self.arrived(stream, step - 1)
            if step < 6:
                self.start(stream, step)

    def drain(self):
        for stream in range(len(ORDERS)):
            for step in range(6):
                for copy in self.copies(stream, step):
                    copy.wait_send()


def ssm_kernel(
    w_hbm, x_hbm, g_hbm, b_hbm, c_hbm, lcol_ref, lrow_ref, whole_ref, before_ref, tail_ref, skip_ref, rate_ref,
    all_ref, dx_ref, dbc_ref, dq_ref,
    w_ref, x_ref, g_ref, b_ref, c_ref, s_all, g_all, s_acc, g_acc, ends, got, dx_all,
    load_sem, own_sem, w_send, w_recv, s_send, s_recv, x_send, x_recv,
):
    chunks = s_all.shape[0]
    parts = got.shape[0]
    width = x_ref.shape[1]
    heads = width // HDIM
    torus = Torus()
    me = lax.axis_index("seq")
    place = lax.axis_index("exp_0") * 4 + lax.axis_index("exp_1")

    def in_part(offset):
        return lax.rem(me + offset, parts)

    def chip_at(index):
        return {"exp_0": lax.div(index, 4), "exp_1": lax.rem(index, 4)}

    pairs_in = ((w_hbm, w_ref), (x_hbm, x_ref), (g_hbm, g_ref), (b_hbm, b_ref), (c_hbm, c_ref))
    loads = [pltpu.make_async_copy(a, b, load_sem.at[k]) for k, (a, b) in enumerate(pairs_in)]
    for load in loads:
        load.start()
    across_y = {"seq": lax.rem(me + 4, 8), "exp_0": 1 - lax.axis_index("exp_0")}
    barrier_with(
        [{"seq": in_part(o)} for o in range(1, parts)]
        + [chip_at(lax.rem(place + o, chunks)) for o in range(1, chunks)]
        + [across_y]
    )
    gather = Gather(torus, w_ref, all_ref, w_send, w_recv)
    streams = range(len(ORDERS))
    loads[0].wait()
    gather.advance(0, streams)
    here = torus.at
    own = pltpu.make_async_copy(w_ref, all_ref.at[here["x"], here["y"], here["z"]], own_sem.at[0])
    own.start()

    def rows_of(chunk):
        return pl.ds(pl.multiple_of(chunk * SPAN, SPAN), SPAN)

    s_acc[...] = jnp.zeros_like(s_acc)
    g_acc[...] = jnp.zeros_like(g_acc)

    def states(chunk, carry):
        rows = rows_of(chunk)
        from_start, to_end = decays(lcol_ref.at[rows])
        fresh = tn(b_ref[rows, :], (x_ref[rows, :].astype(F32) * to_end).astype(BF16))
        back = tn(c_ref[rows, :], (g_ref[rows, :].astype(F32) * from_start).astype(BF16))
        s_all[chunk] = fresh
        g_all[chunk] = back
        s_acc[...] = s_acc[...] * whole_ref[chunk] + fresh
        g_acc[...] = g_acc[...] + before_ref[chunk] * back
        return carry

    for load in loads[1:]:
        load.wait()
    lax.fori_loop(0, chunks, states, 0)
    ends[0, :128, :] = s_acc[...].astype(BF16)
    ends[1, :128, :] = g_acc[...].astype(BF16)
    ends[0, 128:, :] = tail_ref[...]
    ends[1, 128:, :] = tail_ref[...]

    def to_part(offset, back=False):
        peer = in_part(offset)
        source = in_part(parts - offset)
        common = dict(
            send_sem=s_send.at[offset - 1], recv_sem=s_recv.at[offset - 1], device_id={"seq": peer}, device_id_type=MESH
        )
        which = jnp.where(peer > me, 0, 1)
        if back:
            return pltpu.make_async_remote_copy(src_ref=got.at[source], dst_ref=got.at[source], **common)
        return pltpu.make_async_remote_copy(src_ref=ends.at[which], dst_ref=got.at[me], **common)

    for offset in range(1, parts):
        to_part(offset).start()
    own.wait()
    gather.advance(1, streams)
    got[me] = jnp.zeros(got.shape[1:], BF16)
    for offset in range(1, parts):
        to_part(offset, back=True).wait_recv()
    gather.advance(2, streams)

    def decay_of(m):
        return got[m, 128:129, :].astype(F32) + got[m, 129:130, :].astype(F32)

    state = jnp.zeros((128, width), F32)
    for m in range(parts):
        state = jnp.where(m < me, decay_of(m) * state + got[m, :128, :].astype(F32), state)
    for k in range(chunks):
        fresh = s_all[k]
        s_all[k] = state
        state = state * whole_ref[k] + fresh
    state = jnp.zeros((128, width), F32)
    for m in reversed(range(parts)):
        state = jnp.where(m > me, decay_of(m) * state + got[m, :128, :].astype(F32), state)
    for k in reversed(range(chunks)):
        fresh = g_all[k]
        g_all[k] = state
        state = state * whole_ref[k] + fresh

    row = lax.broadcasted_iota(jnp.int32, (SPAN, SPAN), 0)
    col = lax.broadcasted_iota(jnp.int32, (SPAN, SPAN), 1)
    head_of = lax.broadcasted_iota(jnp.int32, (8, width), 1) // HDIM
    pick = (head_of == lax.broadcasted_iota(jnp.int32, (8, width), 0)).astype(F32)
    pick_half = pick.astype(BF16)

    def to_chip(turn, back=False):
        target = lax.rem(place + 1 + turn, chunks)
        source = lax.rem(place + (chunks - 1) - turn, chunks)
        common = dict(
            send_sem=x_send.at[turn], recv_sem=x_recv.at[turn], device_id=chip_at(target), device_id_type=MESH
        )
        if back:
            return pltpu.make_async_remote_copy(src_ref=dx_ref.at[source], dst_ref=dx_ref.at[source], **common)
        return pltpu.make_async_remote_copy(src_ref=dx_all.at[target], dst_ref=dx_ref.at[place], **common)

    def grads(turn, carry):
        chunk = lax.rem(place + 1 + turn, chunks)
        rows = rows_of(chunk)
        x = x_ref[rows, :]
        g = g_ref[rows, :]
        b = b_ref[rows, :]
        c = c_ref[rows, :]
        lcol = lcol_ref[rows, :]
        lrow = lrow_ref[:, rows]
        s_in = s_all[chunk]
        g_out = g_all[chunk]
        s_half = s_in.astype(BF16)
        g_half = g_out.astype(BF16)
        upper = row <= col
        strict = row < col
        from_row = (row >= col).astype(F32).astype(BF16)
        before_row = strict.astype(F32).astype(BF16)
        bc = nt(b, c)
        dx = jnp.zeros((SPAN, width), F32)
        pairs = jnp.zeros((SPAN, SPAN), F32)
        inside = []
        for h in range(heads):
            mine = pick_half[h : h + 1, :]
            m = nt(x * mine, g)
            w = jnp.exp(jnp.where(upper, lcol[:, h : h + 1] - lrow[h : h + 1, :], -1e30))
            a1 = w * bc
            pairs = pairs + w * m
            dx = dx + nn(a1.astype(BF16), g * mine)
            p = jnp.where(strict, a1 * m, 0.0).astype(BF16)
            inside.append(jnp.sum(jnp.where(strict, nn(p, from_row), 0.0), axis=0, keepdims=True))
        from_start, to_end = decays(lcol_ref.at[rows])
        ge = (g.astype(F32) * from_start).astype(BF16)
        xe = (x.astype(F32) * to_end).astype(BF16)
        pairs_half = pairs.astype(BF16)
        z = nn(c, s_half)
        v = nn(b, g_half)
        dbc_ref[rows, :128] = nn(pairs_half, c) + nt(xe, g_half)
        dbc_ref[rows, 128:] = tn(pairs_half, b) + nt(ge, s_half)
        dx_all[chunk] = (dx + to_end * v + skip_ref[...] * g.astype(F32)).astype(BF16)

        @pl.when(turn < chunks - 1)
        def _():
            to_chip(turn).start()

        rc = nt(pick_half, (ge.astype(F32) * z).astype(BF16))
        cc = nt(pick_half, (xe.astype(F32) * v).astype(BF16))
        across = jnp.sum(s_in * g_out, axis=0, keepdims=True) * whole_ref[chunk]
        ones = jnp.ones((width, SPAN), BF16)
        dq = nn(rc.astype(BF16), from_row) + nn(cc.astype(BF16), before_row) + nn((pick * across).astype(BF16), ones)
        for h in range(heads):
            dq_ref[h : h + 1, rows] = -(dq[h : h + 1, :] + inside[h]) * rate_ref[h : h + 1, :]
        for step, after in STEPS_AFTER:

            @pl.when(turn == after)
            def _(step=step):
                gather.advance(step, streams)

        return carry

    lax.fori_loop(0, chunks, grads, 0)
    mine = pltpu.make_async_copy(dx_all.at[place], dx_ref.at[place], own_sem.at[0])
    mine.start()
    for step in LAST_STEPS:
        gather.advance(step, streams)
    mine.wait()
    for turn in range(chunks - 1):
        to_chip(turn, back=True).wait_recv()
        to_chip(turn).wait_send()
    for offset in range(1, parts):
        to_part(offset).wait_send()
    gather.drain()


STEPS_AFTER = ((3, 1), (4, 3))
LAST_STEPS = (5, 6)


def ssm_part(in_weight, ssm_in, b_proj, c_proj, step_sizes, a_log, skip_gain, ssm_grad):
    length, width = ssm_in.shape
    heads = width // HDIM
    chunks = length // SPAN
    parts = lax.axis_size("seq")
    rates = jnp.exp(a_log)
    steps = (step_sizes * rates[:, None]).reshape(heads * chunks, SPAN)
    at = jnp.arange(SPAN)
    lrow = jnp.dot(steps, (at[:, None] <= at[None, :]).astype(F32), precision=lax.Precision.HIGHEST)
    totals = lrow[:, -1].reshape(heads, chunks)
    lrow = lrow.reshape(heads, length)
    lcol = lrow.T
    whole = jnp.repeat(jnp.exp(-totals).T, HDIM, axis=1).reshape(chunks, 1, width)
    sums = jnp.cumsum(totals, axis=1)
    before = jnp.repeat(jnp.exp(-(sums - totals)).T, HDIM, axis=1).reshape(chunks, 1, width)
    device_decay = jnp.repeat(jnp.exp(-sums[:, -1]), HDIM)
    skip = jnp.repeat(skip_gain, HDIM).reshape(1, width)
    high = device_decay.astype(BF16)
    low = (device_decay - high.astype(F32)).astype(BF16)
    tail = jnp.pad(jnp.stack([high, low]), ((0, 14), (0, 0)))
    vmem = pl.BlockSpec(memory_space=pltpu.VMEM)
    hbm = pl.BlockSpec(memory_space=pl.ANY)
    streams = len(ORDERS)
    dma = pltpu.SemaphoreType.DMA
    return pl.pallas_call(
        ssm_kernel,
        out_shape=(
            jax.ShapeDtypeStruct((4, 4, 4, *in_weight.shape), BF16),
            jax.ShapeDtypeStruct((chunks, SPAN, width), BF16),
            jax.ShapeDtypeStruct((length, 256), F32),
            jax.ShapeDtypeStruct((heads, length), F32),
        ),
        in_specs=[pl.BlockSpec(memory_space=pltpu.HBM)] * 5 + [vmem] * 7,
        out_specs=(hbm, hbm, vmem, vmem),
        scratch_shapes=[
            pltpu.VMEM(in_weight.shape, BF16),
            pltpu.VMEM((length, width), BF16),
            pltpu.VMEM((length, width), BF16),
            pltpu.VMEM((length, 128), BF16),
            pltpu.VMEM((length, 128), BF16),
            pltpu.VMEM((chunks, 128, width), F32),
            pltpu.VMEM((chunks, 128, width), F32),
            pltpu.VMEM((128, width), F32),
            pltpu.VMEM((128, width), F32),
            pltpu.VMEM((2, 144, width), BF16),
            pltpu.VMEM((parts, 144, width), BF16),
            pltpu.VMEM((chunks, SPAN, width), BF16),
            dma((5,)),
            dma((1,)),
            dma((streams, 6, 2)),
            dma((streams, 6, 2)),
            dma((parts - 1,)),
            dma((parts - 1,)),
            dma((chunks - 1,)),
            dma((chunks - 1,)),
        ],
        compiler_params=pltpu.CompilerParams(
            collective_id=1, has_side_effects=True, vmem_limit_bytes=48 * 2**20
        ),
        name="ssm",
    )(in_weight, ssm_in, ssm_grad, b_proj, c_proj, lcol, lrow, whole, before, tail, skip, rates[:, None])


def project_kernel(core_ref, x_ref, w_ref, keep_ref, send_ref, total):
    core = core_ref[0]
    half = keep_ref.shape[0]
    width = x_ref.shape[2]
    acc = jnp.zeros(total.shape, F32)
    for k in range(x_ref.shape[0]):
        acc = acc + nt(x_ref[k], w_ref[0, k // 4, 0, k % 4])
    total[...] = acc
    keep_ref[...] = total[pl.ds(pl.multiple_of(core * half, half), half), :].astype(BF16)
    send_ref[...] = total[pl.ds(pl.multiple_of((1 - core) * half, half), half), :].astype(BF16)


def project(x_all, w_all):
    blocks, tokens, width = x_all.shape
    rows = w_all.shape[3]
    w_all = w_all.reshape(4, 2, 2, 4, rows, width)
    half = jax.ShapeDtypeStruct((tokens // 2, 8 * rows), BF16)
    return pl.pallas_call(
        project_kernel,
        grid=(8,),
        out_shape=(half, half),
        in_specs=[
            pl.BlockSpec(memory_space=pltpu.SMEM),
            pl.BlockSpec((blocks, tokens, width), lambda i: (0, 0, 0)),
            pl.BlockSpec((1, 2, 1, 4, rows, width), lambda i: (i % 4, 0, i // 4, 0, 0, 0)),
        ],
        out_specs=(pl.BlockSpec((tokens // 2, rows), lambda i: (0, i)),) * 2,
        scratch_shapes=[pltpu.VMEM((tokens, rows), F32)],
        compiler_params=pltpu.CompilerParams(dimension_semantics=("arbitrary",)),
        name="project",
    )(lax.axis_index(CORE).reshape(1).astype(jnp.int32), x_all, w_all)

def exactly(values, ones):
    high = values.astype(BF16)
    low = (values - high.astype(F32)).astype(BF16)
    ones = ones.astype(F32).astype(BF16)
    return nn(high, ones) + nn(low, ones)


def offset_of(turn):
    j = lax.rem(turn, 4)
    return lax.div(turn, 4), j + lax.div(j, 2) * (1 - 2 * lax.rem(j, 2))


FIRST_COLUMNS = 1792


def expert_kernel(
    keep_ref, other_ref, residual_ref, select_ref, gate_ref, w_hbm, saved_hbm,
    pre_hbm, route_ref,
    rows_out, held, w_ref, saved_buf, pre_buf, shares, part_out, part_in, sum_out, sum_in,
    w_sem, saved_sem, pre_sem, a_send, a_recv, g_send, g_recv, p_send, p_recv, q_send, q_recv,
):
    turns, _, _, block, d = held.shape
    slots = block // 2
    hidden = w_ref.shape[0]
    seq = lax.axis_index("seq")
    x, y = lax.rem(seq, 4), lax.div(seq, 4)
    chip_y, chip_z, core = (lax.axis_index(name) for name in EXP)
    right = {"seq": y * 4 + lax.rem(x + 1, 4)}
    left = {"seq": y * 4 + lax.rem(x + 3, 4)}
    facing = {"seq": lax.rem(seq + 4, 8)}
    x_left, x_right, x_far = lax.rem(x + 3, 4), lax.rem(x + 1, 4), lax.rem(x + 2, 4)
    mates = [{"exp_2": 1 - core}]
    for turn in range(1, turns):
        by, bz = turn // 4, (0, 1, 3, 2)[turn % 4]
        for k in range(2):
            mates.append(
                {
                    "seq": lax.rem(seq + 4 * by, 8),
                    "exp_0": lax.rem(chip_y + by, 2),
                    "exp_1": lax.rem(chip_z + (4 - bz), 4),
                    "exp_2": k,
                }
            )
    mates += [{"seq": lax.rem(seq + k, 8)} for k in range(1, 8)]
    mates += [{"exp_0": 1 - chip_y, "exp_1": z, "exp_2": k} for z in range(4) for k in range(2)]
    barrier_with(mates)
    load_w = pltpu.make_async_copy(w_hbm.at[0], w_ref, w_sem.at[0])
    load_w.start()

    def chip_of(turn):
        by, bz = offset_of(turn)
        return lax.rem(chip_y + by, 2) * 4 + lax.rem(chip_z + bz, 4)

    def load_saved(turn):
        slot = lax.rem(turn, 2)
        return pltpu.make_async_copy(saved_hbm.at[:, chip_of(turn)], saved_buf.at[slot], saved_sem.at[slot])

    def store_pre(turn):
        slot = lax.rem(turn, 2)
        return pltpu.make_async_copy(pre_buf.at[slot], pre_hbm.at[:, chip_of(turn)], pre_sem.at[slot])

    load_saved(0).start()
    moe = (residual_ref[...].astype(F32) + keep_ref[...].astype(F32) + other_ref[...].astype(F32)).astype(BF16)
    rows = (nn(select_ref[...], moe) * gate_ref[...]).astype(BF16)
    rows_out[...] = rows.reshape(rows_out.shape)
    half_of = lambda c: pl.ds(pl.multiple_of(c * slots, slots), slots)

    def first_of(turn):
        return lax.rem(y + lax.div(turn, 4), 2)

    def to_expert(turn, k):
        by, bz = turn // 4, (0, 1, 3, 2)[turn % 4]
        ty, tz = lax.rem(chip_y + by, 2), lax.rem(chip_z + (4 - bz), 4)
        return pltpu.make_async_remote_copy(
            src_ref=rows_out.at[(ty * 4 + tz) * 2 + k],
            dst_ref=held.at[turn, y, x, half_of(core)],
            send_sem=a_send.at[turn, k],
            recv_sem=a_recv.at[turn, core],
            device_id={"seq": lax.rem(seq + 4 * by, 8), "exp_0": ty, "exp_1": tz, "exp_2": k},
            device_id_type=MESH,
        )

    def from_source(turn, c):
        there = held.at[turn, first_of(turn), x, half_of(c)]
        return pltpu.make_async_remote_copy(
            src_ref=there, dst_ref=there, send_sem=a_send.at[turn, 0], recv_sem=a_recv.at[turn, c],
            device_id={"exp_2": 1 - core}, device_id_type=MESH,
        )

    to_expert(0, 1 - core).start()
    for turn in range(1, turns):
        for k in range(2):
            to_expert(turn, k).start()
    held[0, y, x, half_of(core), :] = rows_out[(chip_y * 4 + chip_z) * 2 + core]

    first = pl.ds(0, FIRST_COLUMNS)
    rest = pl.ds(FIRST_COLUMNS, d - FIRST_COLUMNS)
    low, high, both = pl.ds(0, slots), pl.ds(slots, slots), slice(None)

    def moves(i, step):
        start = first_of(i)
        if step == 0:
            return (
                (0, held.at[i, start, x, both, first], held.at[i, start, x_left, both, first], right),
                (1, held.at[i, start, x, both, first], held.at[i, start, x_right, both, first], left),
                (2, held.at[i, start, x, both, rest], held.at[i, 1 - start, x, both, rest], facing),
            )
        if step == 1:
            return (
                (3, held.at[i, start, x_left, low, first], held.at[i, start, x_far, low, first], right),
                (4, held.at[i, start, x_right, high, first], held.at[i, start, x_far, high, first], left),
                (5, held.at[i, both, x, both, rest], held.at[i, both, x_left, both, rest], right),
                (6, held.at[i, both, x, both, rest], held.at[i, both, x_right, both, rest], left),
            )
        return (
            (7, held.at[i, start, both, both, first], held.at[i, 1 - start, both, both, first], facing),
            (8, held.at[i, both, x_left, low, rest], held.at[i, both, x_far, low, rest], right),
            (9, held.at[i, both, x_right, high, rest], held.at[i, both, x_far, high, rest], left),
        )

    def each(i, step, act):
        for number, sent, arriving, peer in moves(i, step):
            ref = arriving if act == "wait_recv" else sent
            copy = pltpu.make_async_remote_copy(
                src_ref=ref, dst_ref=ref, send_sem=g_send.at[i, number], recv_sem=g_recv.at[i, number],
                device_id=peer, device_id_type=MESH,
            )
            getattr(copy, act)()

    def compute(j):
        slot = lax.rem(j, 2)
        load_saved(j).wait()

        @pl.when(j < turns - 1)
        def _():
            load_saved(j + 1).start()

        @pl.when(j >= 2)
        def _():
            store_pre(j - 2).wait()

        count = 8 * block
        upstream = nt(held[j].reshape(count, d), w_ref[...])
        gate_pre = saved_buf[slot, :, :, 0, :].astype(F32).reshape(count, hidden)
        up_pre = saved_buf[slot, :, :, 1, :].astype(F32).reshape(count, hidden)
        sig = jax.nn.sigmoid(gate_pre)
        act = gate_pre * sig
        up_grad = upstream * act
        gate_grad = upstream * up_pre * sig * (1.0 + gate_pre * (1.0 - sig))
        pre_buf[slot, :, :, 0, :] = gate_grad.astype(BF16).reshape(8, block, hidden)
        pre_buf[slot, :, :, 1, :] = up_grad.astype(BF16).reshape(8, block, hidden)
        store_pre(j).start()
        sums = nt(jnp.ones((8, hidden), BF16), (up_grad * up_pre).astype(BF16))
        at = lambda dim, *shape: lax.broadcasted_iota(jnp.int32, shape, dim)
        sums = jnp.where(lax.div(at(1, 8, count), block) == at(0, 8, count), sums, 0.0)
        shares[...] += exactly(
            sums, lax.rem(at(0, count, turns * block), block) + chip_of(j) * block == at(1, count, turns * block)
        )

    def pass_on(t, carry):
        @pl.when(t == 0)
        def _():
            from_source(0, 1 - core).wait_recv()
            each(0, 0, "start")

        @pl.when(jnp.logical_and(t >= 1, t < turns))
        def _():
            for c in range(2):
                from_source(t, c).wait_recv()
            each(t, 0, "start")

        @pl.when(jnp.logical_and(t >= 1, t < turns + 1))
        def _():
            each(t - 1, 0, "wait_recv")
            each(t - 1, 1, "start")

        @pl.when(jnp.logical_and(t >= 2, t < turns + 2))
        def _():
            each(t - 2, 1, "wait_recv")
            each(t - 2, 2, "start")

        @pl.when(t == 2)
        def _():
            load_w.wait()

        @pl.when(t >= 3)
        def _():
            each(t - 3, 2, "wait_recv")
            compute(t - 3)

        return carry

    shares[...] = jnp.zeros_like(shares)
    lax.fori_loop(0, turns + 3, pass_on, 0)
    all_exp = 16
    own = (chip_y * 4 + chip_z) * 2 + core

    def exp_device(index):
        return {"exp_0": lax.div(index, 8), "exp_1": lax.rem(lax.div(index, 2), 4), "exp_2": lax.rem(index, 2)}

    def part(k, back=False):
        to, source = lax.rem(seq + k, 8), lax.rem(seq + (8 - k), 8)
        return pltpu.make_async_remote_copy(
            src_ref=part_in.at[source] if back else part_out.at[to],
            dst_ref=part_in.at[source] if back else part_in.at[seq],
            send_sem=p_send.at[k - 1], recv_sem=p_recv.at[k - 1], device_id={"seq": to}, device_id_type=MESH,
        )

    def total(k, back=False):
        to, source = lax.rem(own + k, all_exp), lax.rem(own + (all_exp - k), all_exp)
        return pltpu.make_async_remote_copy(
            src_ref=sum_in.at[source] if back else sum_out.at[to],
            dst_ref=sum_in.at[source] if back else sum_in.at[own],
            send_sem=q_send.at[k - 1], recv_sem=q_recv.at[k - 1], device_id=exp_device(to), device_id_type=MESH,
        )

    for k in range(8):
        part_out[k] = shares[k : k + 1, :]
    for k in range(1, 8):
        part(k).start()
    part_in[seq] = part_out[seq]
    for k in range(1, 8):
        part(k, back=True).wait_recv()
    summed = part_in[0]
    for k in range(1, 8):
        summed = summed + part_in[k]
    at = lambda dim, *shape: lax.broadcasted_iota(jnp.int32, shape, dim)
    width = summed.shape[1]
    each_exp = jnp.where(lax.div(at(1, all_exp, width), slots) == at(0, all_exp, width), summed, 0.0)
    each_exp = exactly(each_exp, lax.rem(at(0, width, 128), slots) == at(1, width, 128))
    for k in range(all_exp):
        sum_out[k] = each_exp[k : k + 1, :]
    for k in range(1, all_exp):
        total(k).start()
    sum_in[own] = sum_out[own]
    for k in range(1, all_exp):
        total(k, back=True).wait_recv()
    for k in range(all_exp):
        route_ref[k : k + 1, :] = sum_in[k]
    for k in range(1, 8):
        part(k).wait_send()
    for k in range(1, all_exp):
        total(k).wait_send()
    store_pre(turns - 2).wait()
    store_pre(turns - 1).wait()
    to_expert(0, 1 - core).wait_send()
    for turn in range(1, turns):
        for k in range(2):
            to_expert(turn, k).wait_send()

    def sent(i, carry):
        for step in range(3):
            each(i, step, "wait_send")
        return carry

    lax.fori_loop(0, turns, sent, 0)


def expert_part(keep, other, residual, select, slot_gates, w_down, saved_pre):
    slots, _, hidden = saved_pre.shape[1:]
    d = residual.shape[1]
    rows = select.shape[0]
    turns, block = 8, rows // 8
    vmem = pl.BlockSpec(memory_space=pltpu.VMEM)
    hbm = pl.BlockSpec(memory_space=pl.ANY)
    dma = pltpu.SemaphoreType.DMA
    pre, route = pl.pallas_call(
        expert_kernel,
        out_shape=(
            jax.ShapeDtypeStruct((8, turns, block, 2, hidden), BF16),
            jax.ShapeDtypeStruct((16, 128), F32),
        ),
        in_specs=[vmem] * 5 + [hbm] * 2,
        out_specs=(hbm, vmem),
        scratch_shapes=[
            pltpu.VMEM((16, rows // 16, d), BF16),
            pltpu.VMEM((turns, 2, 4, block, d), BF16),
            pltpu.VMEM((hidden, d), BF16),
            pltpu.VMEM((2, 8, block, 2, hidden), BF16),
            pltpu.VMEM((2, 8, block, 2, hidden), BF16),
            pltpu.VMEM((8, turns * block), F32),
            pltpu.VMEM((8, 1, turns * block), F32),
            pltpu.VMEM((8, 1, turns * block), F32),
            pltpu.VMEM((16, 1, 128), F32),
            pltpu.VMEM((16, 1, 128), F32),
            dma((1,)),
            dma((2,)),
            dma((2,)),
            dma((turns, 2)),
            dma((turns, 2)),
            dma((turns, 10)),
            dma((turns, 10)),
            dma((7,)),
            dma((7,)),
            dma((15,)),
            dma((15,)),
        ],
        compiler_params=pltpu.CompilerParams(
            collective_id=2, has_side_effects=True, vmem_limit_bytes=60 * 2**20
        ),
        name="experts",
    )(keep, other, residual, select, slot_gates, w_down, saved_pre.reshape(8, turns, block, 2, hidden))
    return pre.reshape(saved_pre.shape), route[:, : block // 2].reshape(-1)


def per_device(
    gates, expert_ids, saved_pre, w_down, residual_grad, in_weight, ssm_in, b_proj, c_proj, step_sizes, a_log, skip_gain, ssm_grad
):
    w_all, x_all, bc_grads, step_grads = ssm_part(
        in_weight, ssm_in, b_proj, c_proj, step_sizes, a_log, skip_gain, ssm_grad
    )
    tokens_here = residual_grad.shape[0]
    experts = lax.axis_size(EXP)
    capacity = TOPK * tokens_here // experts
    bc_grads = lax.psum_scatter(bc_grads, EXP, scatter_dimension=0, tiled=True)
    b_grads, c_grads = bc_grads[:, :128], bc_grads[:, 128:]
    keep, send = project(x_all, w_all)
    other = lax.ppermute(send, CORE, [(0, 1), (1, 0)])
    flat_ids = expert_ids.reshape(-1)
    onehot = (flat_ids[:, None] == jnp.arange(experts, dtype=jnp.int32)[None, :]).astype(jnp.int32)
    position = jnp.sum(onehot * jnp.cumsum(onehot, axis=0), axis=1) - 1
    target = flat_ids * capacity + position
    selector = target[:, None] == jnp.arange(experts * capacity, dtype=jnp.int32)[None, :]
    by_token = selector.reshape(tokens_here, TOPK, -1)
    slot_gates = jnp.sum(by_token * gates[:, :, None], axis=(0, 1))
    select = jnp.any(by_token, axis=1).astype(BF16).T
    pre_grads, totals = expert_part(keep, other, residual_grad, select, slot_gates[:, None], w_down, saved_pre)
    route_grads = totals[target].reshape(tokens_here, TOPK) / gates
    return (pre_grads, route_grads, b_grads, c_grads, step_grads)


def solution(mesh):
    split = Mesh(mesh.devices.reshape(mesh.shape["seq"], 2, 4, 2), ("seq", "exp_0", "exp_1", "exp_2"))
    in_specs = (
        P(SEQ_EXP, None), P(SEQ_EXP, None), P(EXP, None, None, "seq"), P(EXP, "seq", None), P(SEQ_EXP, None), P("seq", EXP),
        P("seq", EXP), P("seq", None), P("seq", None), P(EXP, "seq"), P(EXP), P(EXP), P("seq", EXP),
    )
    out_specs = (P(EXP, None, None, "seq"), P(SEQ_EXP, None), P(SEQ_EXP, None), P(SEQ_EXP, None), P(EXP, "seq"))
    return jax.shard_map(per_device, mesh=split, in_specs=in_specs, out_specs=out_specs, check_vma=False)
```

```python
import functools

import jax
import jax.numpy as jnp
from jax import lax
from jax.experimental import pallas as pl
from jax.experimental.pallas import tpu as pltpu
from jax.sharding import Mesh
from jax.sharding import PartitionSpec as P

TOPK = 2
HDIM = 64
SPAN = 256
CHIPS = ("exp_0", "exp_1")
CORE = "exp_2"
EXP = ("exp_0", "exp_1", "exp_2")
SEQ_EXP = ("seq", "exp_0", "exp_1", "exp_2")
F32 = jnp.float32
BF16 = jnp.bfloat16
MESH = pl.DeviceIdType.MESH


def nn(a, b):
    return lax.dot_general(a, b, (((1,), (0,)), ((), ())), preferred_element_type=F32)


def nt(a, b):
    return lax.dot_general(a, b, (((1,), (1,)), ((), ())), preferred_element_type=F32)


def tn(a, b):
    return lax.dot_general(a, b, (((0,), (0,)), ((), ())), preferred_element_type=F32)


def over_lanes(columns):
    rows, heads = columns.shape
    lane = lax.broadcasted_iota(jnp.int32, (rows, 2 * HDIM), 1)
    return jnp.concatenate(
        [
            jnp.where(lane < HDIM, columns[:, h : h + 1], columns[:, h + 1 : h + 2])
            for h in range(0, heads, 2)
        ],
        axis=1,
    )


def decays(lcol_ref):
    running = lcol_ref[...]
    last = running[SPAN - 1 : SPAN, :]
    return over_lanes(jnp.exp(-running)), over_lanes(jnp.exp(running - last))


def barrier_with(peers):
    semaphore = pltpu.get_barrier_semaphore()
    for peer in peers:
        pl.semaphore_signal(semaphore, inc=1, device_id=peer, device_id_type=MESH)
    pl.semaphore_wait(semaphore, len(peers))


ORDERS = ("xyz", "yzx", "zxy", "xzy", "yxz", "zyx")
SHARES = (5, 6, 5, 5, 5, 6)
UNIT = 16


class Torus:
    def __init__(self):
        seq = lax.axis_index("seq")
        self.at = {
            "x": lax.rem(seq, 4),
            "y": lax.axis_index("exp_0") * 2 + lax.div(seq, 4),
            "z": lax.axis_index("exp_1"),
        }

    def device(self, dim, step):
        at = dict(self.at)
        at[dim] = lax.rem(at[dim] + (step + 4), 4)
        return {"seq": lax.rem(at["y"], 2) * 4 + at["x"], "exp_0": lax.div(at["y"], 2), "exp_1": at["z"]}


class Gather:
    def __init__(self, torus, own_ref, out_ref, send_sem, recv_sem):
        self.torus, self.own, self.out = torus, own_ref, out_ref
        self.send_sem, self.recv_sem = send_sem, recv_sem
        self.rows = [(sum(SHARES[:k]) * UNIT, SHARES[k] * UNIT) for k in range(len(ORDERS))]

    def block(self, stream, phase, step, start, size):
        order = ORDERS[stream]
        at = []
        for dim in "xyz":
            k = order.index(dim)
            if k < phase:
                at.append(slice(None))
            elif k == phase:
                at.append(lax.rem(self.torus.at[dim] + (step + 4), 4))
            else:
                at.append(self.torus.at[dim])
        return self.out.at[(*at, pl.ds(start, size), slice(None))]

    def copies(self, stream, step, back=False):
        phase, second = step // 2, step % 2
        dim = ORDERS[stream][phase]
        start, size = self.rows[stream]
        half = (size // UNIT + 1) // 2 * UNIT
        made = []
        for side, way in enumerate((1, -1)):
            if not second:
                span, hop = (start, size), 0
            else:
                span = (start, half) if side == 0 else (start + half, size - half)
                hop = -way
            sent = self.block(stream, phase, hop, *span)
            here = sent
            if step == 0:
                sent = self.own.at[pl.ds(*span), :]
            common = dict(
                send_sem=self.send_sem.at[stream, step, side],
                recv_sem=self.recv_sem.at[stream, step, side],
                device_id=self.torus.device(dim, way),
                device_id_type=MESH,
            )
            if back:
                sent = here = self.block(stream, phase, hop - way, *span)
            made.append(pltpu.make_async_remote_copy(src_ref=sent, dst_ref=here, **common))
        return made

    def start(self, stream, step):
        for copy in self.copies(stream, step):
            copy.start()

    def arrived(self, stream, step):
        for copy in self.copies(stream, step, back=True):
            copy.wait_recv()

    def advance(self, step, streams):
        for stream in streams:
            if step > 0:
                self.arrived(stream, step - 1)
            if step < 6:
                self.start(stream, step)

    def drain(self):
        for stream in range(len(ORDERS)):
            for step in range(6):
                for copy in self.copies(stream, step):
                    copy.wait_send()


def ssm_kernel(
    w_hbm, x_hbm, g_hbm, b_hbm, c_hbm, lcol_ref, lrow_ref, whole_ref, before_ref, tail_ref, skip_ref, rate_ref,
    all_ref, dx_ref, dbc_ref, dq_ref,
    w_ref, x_ref, g_ref, b_ref, c_ref, s_all, g_all, s_acc, g_acc, ends, got, dx_all,
    load_sem, own_sem, w_send, w_recv, s_send, s_recv, x_send, x_recv,
):
    chunks = s_all.shape[0]
    parts = got.shape[0]
    width = x_ref.shape[1]
    heads = width // HDIM
    torus = Torus()
    me = lax.axis_index("seq")
    place = lax.axis_index("exp_0") * 4 + lax.axis_index("exp_1")

    def in_part(offset):
        return lax.rem(me + offset, parts)

    def chip_at(index):
        return {"exp_0": lax.div(index, 4), "exp_1": lax.rem(index, 4)}

    pairs_in = ((w_hbm, w_ref), (x_hbm, x_ref), (g_hbm, g_ref), (b_hbm, b_ref), (c_hbm, c_ref))
    loads = [pltpu.make_async_copy(a, b, load_sem.at[k]) for k, (a, b) in enumerate(pairs_in)]
    for load in loads:
        load.start()
    across_y = {"seq": lax.rem(me + 4, 8), "exp_0": 1 - lax.axis_index("exp_0")}
    barrier_with(
        [{"seq": in_part(o)} for o in range(1, parts)]
        + [chip_at(lax.rem(place + o, chunks)) for o in range(1, chunks)]
        + [across_y]
    )
    gather = Gather(torus, w_ref, all_ref, w_send, w_recv)
    streams = range(len(ORDERS))
    loads[0].wait()
    gather.advance(0, streams)
    here = torus.at
    own = pltpu.make_async_copy(w_ref, all_ref.at[here["x"], here["y"], here["z"]], own_sem.at[0])
    own.start()

    def rows_of(chunk):
        return pl.ds(pl.multiple_of(chunk * SPAN, SPAN), SPAN)

    s_acc[...] = jnp.zeros_like(s_acc)
    g_acc[...] = jnp.zeros_like(g_acc)

    def states(chunk, carry):
        @pl.when(chunk == 3)
        def _():
            gather.advance(1, streams)

        rows = rows_of(chunk)
        from_start, to_end = decays(lcol_ref.at[rows])
        fresh = tn(b_ref[rows, :], (x_ref[rows, :].astype(F32) * to_end).astype(BF16))
        back = tn(c_ref[rows, :], (g_ref[rows, :].astype(F32) * from_start).astype(BF16))
        s_all[chunk] = fresh
        g_all[chunk] = back
        s_acc[...] = s_acc[...] * whole_ref[chunk] + fresh
        g_acc[...] = g_acc[...] + before_ref[chunk] * back
        return carry

    for load in loads[1:]:
        load.wait()
    lax.fori_loop(0, chunks, states, 0)
    ends[0, :128, :] = s_acc[...].astype(BF16)
    ends[1, :128, :] = g_acc[...].astype(BF16)
    ends[0, 128:, :] = tail_ref[...]
    ends[1, 128:, :] = tail_ref[...]

    def to_part(offset, back=False):
        peer = in_part(offset)
        source = in_part(parts - offset)
        common = dict(
            send_sem=s_send.at[offset - 1], recv_sem=s_recv.at[offset - 1], device_id={"seq": peer}, device_id_type=MESH
        )
        which = jnp.where(peer > me, 0, 1)
        if back:
            return pltpu.make_async_remote_copy(src_ref=got.at[source], dst_ref=got.at[source], **common)
        return pltpu.make_async_remote_copy(src_ref=ends.at[which], dst_ref=got.at[me], **common)

    for offset in range(1, parts):
        to_part(offset).start()
    own.wait()
    gather.advance(2, streams)
    got[me] = jnp.zeros(got.shape[1:], BF16)
    for offset in range(1, parts):
        to_part(offset, back=True).wait_recv()

    def decay_of(m):
        return got[m, 128:129, :].astype(F32) + got[m, 129:130, :].astype(F32)

    state = jnp.zeros((128, width), F32)
    for m in range(parts):
        state = jnp.where(m < me, decay_of(m) * state + got[m, :128, :].astype(F32), state)
    for k in range(chunks):
        fresh = s_all[k]
        s_all[k] = state
        state = state * whole_ref[k] + fresh
    state = jnp.zeros((128, width), F32)
    for m in reversed(range(parts)):
        state = jnp.where(m > me, decay_of(m) * state + got[m, :128, :].astype(F32), state)
    for k in reversed(range(chunks)):
        fresh = g_all[k]
        g_all[k] = state
        state = state * whole_ref[k] + fresh

    row = lax.broadcasted_iota(jnp.int32, (SPAN, SPAN), 0)
    col = lax.broadcasted_iota(jnp.int32, (SPAN, SPAN), 1)
    head_of = lax.broadcasted_iota(jnp.int32, (8, width), 1) // HDIM
    pick = (head_of == lax.broadcasted_iota(jnp.int32, (8, width), 0)).astype(F32)
    pick_half = pick.astype(BF16)

    def to_chip(turn, back=False):
        target = lax.rem(place + 1 + turn, chunks)
        source = lax.rem(place + (chunks - 1) - turn, chunks)
        common = dict(
            send_sem=x_send.at[turn], recv_sem=x_recv.at[turn], device_id=chip_at(target), device_id_type=MESH
        )
        if back:
            return pltpu.make_async_remote_copy(src_ref=dx_ref.at[source], dst_ref=dx_ref.at[source], **common)
        return pltpu.make_async_remote_copy(src_ref=dx_all.at[target], dst_ref=dx_ref.at[place], **common)

    def grads(turn, carry):
        chunk = lax.rem(place + 1 + turn, chunks)
        rows = rows_of(chunk)
        x = x_ref[rows, :]
        g = g_ref[rows, :]
        b = b_ref[rows, :]
        c = c_ref[rows, :]
        lcol = lcol_ref[rows, :]
        lrow = lrow_ref[:, rows]
        s_in = s_all[chunk]
        g_out = g_all[chunk]
        s_half = s_in.astype(BF16)
        g_half = g_out.astype(BF16)
        upper = row <= col
        strict = row < col
        from_row = (row >= col).astype(F32).astype(BF16)
        before_row = strict.astype(F32).astype(BF16)
        bc = nt(b, c)
        dx = jnp.zeros((SPAN, width), F32)
        pairs = jnp.zeros((SPAN, SPAN), F32)
        inside = []
        for h in range(heads):
            mine = pick_half[h : h + 1, :]
            m = nt(x * mine, g)
            w = jnp.exp(jnp.where(upper, lcol[:, h : h + 1] - lrow[h : h + 1, :], -1e30))
            a1 = w * bc
            pairs = pairs + w * m
            dx = dx + nn(a1.astype(BF16), g * mine)
            p = jnp.where(strict, a1 * m, 0.0).astype(BF16)
            inside.append(jnp.sum(jnp.where(strict, nn(p, from_row), 0.0), axis=0, keepdims=True))
        from_start, to_end = decays(lcol_ref.at[rows])
        ge = (g.astype(F32) * from_start).astype(BF16)
        xe = (x.astype(F32) * to_end).astype(BF16)
        pairs_half = pairs.astype(BF16)
        z = nn(c, s_half)
        v = nn(b, g_half)
        dbc_ref[rows, :128] = (nn(pairs_half, c) + nt(xe, g_half)).astype(BF16)
        dbc_ref[rows, 128:] = (tn(pairs_half, b) + nt(ge, s_half)).astype(BF16)
        dx_all[chunk] = (dx + to_end * v + skip_ref[...] * g.astype(F32)).astype(BF16)

        @pl.when(turn < chunks - 1)
        def _():
            to_chip(turn).start()

        rc = nt(pick_half, (ge.astype(F32) * z).astype(BF16))
        cc = nt(pick_half, (xe.astype(F32) * v).astype(BF16))
        across = jnp.sum(s_in * g_out, axis=0, keepdims=True) * whole_ref[chunk]
        ones = jnp.ones((width, SPAN), BF16)
        dq = nn(rc.astype(BF16), from_row) + nn(cc.astype(BF16), before_row) + nn((pick * across).astype(BF16), ones)
        for h in range(heads):
            dq_ref[h : h + 1, rows] = -(dq[h : h + 1, :] + inside[h]) * rate_ref[h : h + 1, :]
        for step, after in STEPS_AFTER:

            @pl.when(turn == after)
            def _(step=step):
                gather.advance(step, streams)

        return carry

    lax.fori_loop(0, chunks, grads, 0)
    mine = pltpu.make_async_copy(dx_all.at[place], dx_ref.at[place], own_sem.at[0])
    mine.start()
    for step in LAST_STEPS:
        gather.advance(step, streams)
    mine.wait()
    for turn in range(chunks - 1):
        to_chip(turn, back=True).wait_recv()
        to_chip(turn).wait_send()
    for offset in range(1, parts):
        to_part(offset).wait_send()
    gather.drain()


STEPS_AFTER = ((3, 0), (4, 3))
LAST_STEPS = (5, 6)


def ssm_part(in_weight, ssm_in, b_proj, c_proj, step_sizes, a_log, skip_gain, ssm_grad):
    length, width = ssm_in.shape
    heads = width // HDIM
    chunks = length // SPAN
    parts = lax.axis_size("seq")
    rates = jnp.exp(a_log)
    steps = (step_sizes * rates[:, None]).reshape(heads * chunks, SPAN)
    at = jnp.arange(SPAN)
    lrow = jnp.dot(steps, (at[:, None] <= at[None, :]).astype(F32), precision=lax.Precision.HIGHEST)
    totals = lrow[:, -1].reshape(heads, chunks)
    lrow = lrow.reshape(heads, length)
    lcol = lrow.T
    whole = jnp.repeat(jnp.exp(-totals).T, HDIM, axis=1).reshape(chunks, 1, width)
    sums = jnp.cumsum(totals, axis=1)
    before = jnp.repeat(jnp.exp(-(sums - totals)).T, HDIM, axis=1).reshape(chunks, 1, width)
    device_decay = jnp.repeat(jnp.exp(-sums[:, -1]), HDIM)
    skip = jnp.repeat(skip_gain, HDIM).reshape(1, width)
    high = device_decay.astype(BF16)
    low = (device_decay - high.astype(F32)).astype(BF16)
    tail = jnp.pad(jnp.stack([high, low]), ((0, 14), (0, 0)))
    vmem = pl.BlockSpec(memory_space=pltpu.VMEM)
    hbm = pl.BlockSpec(memory_space=pl.ANY)
    streams = len(ORDERS)
    dma = pltpu.SemaphoreType.DMA
    return pl.pallas_call(
        ssm_kernel,
        out_shape=(
            jax.ShapeDtypeStruct((4, 4, 4, *in_weight.shape), BF16),
            jax.ShapeDtypeStruct((chunks, SPAN, width), BF16),
            jax.ShapeDtypeStruct((length, 256), BF16),
            jax.ShapeDtypeStruct((heads, length), F32),
        ),
        in_specs=[pl.BlockSpec(memory_space=pltpu.HBM)] * 5 + [vmem] * 7,
        out_specs=(hbm, hbm, vmem, vmem),
        scratch_shapes=[
            pltpu.VMEM(in_weight.shape, BF16),
            pltpu.VMEM((length, width), BF16),
            pltpu.VMEM((length, width), BF16),
            pltpu.VMEM((length, 128), BF16),
            pltpu.VMEM((length, 128), BF16),
            pltpu.VMEM((chunks, 128, width), F32),
            pltpu.VMEM((chunks, 128, width), F32),
            pltpu.VMEM((128, width), F32),
            pltpu.VMEM((128, width), F32),
            pltpu.VMEM((2, 144, width), BF16),
            pltpu.VMEM((parts, 144, width), BF16),
            pltpu.VMEM((chunks, SPAN, width), BF16),
            dma((5,)),
            dma((1,)),
            dma((streams, 6, 2)),
            dma((streams, 6, 2)),
            dma((parts - 1,)),
            dma((parts - 1,)),
            dma((chunks - 1,)),
            dma((chunks - 1,)),
        ],
        compiler_params=pltpu.CompilerParams(
            collective_id=1, has_side_effects=True, vmem_limit_bytes=63 * 2**20
        ),
        name="ssm",
    )(in_weight, ssm_in, ssm_grad, b_proj, c_proj, lcol, lrow, whole, before, tail, skip, rates[:, None])


def project_kernel(core_ref, x_ref, w_ref, keep_ref, send_ref, total):
    core = core_ref[0]
    half = keep_ref.shape[0]
    width = x_ref.shape[2]
    acc = jnp.zeros(total.shape, F32)
    for k in range(x_ref.shape[0]):
        acc = acc + nt(x_ref[k], w_ref[0, k // 4, 0, k % 4])
    total[...] = acc
    keep_ref[...] = total[pl.ds(pl.multiple_of(core * half, half), half), :].astype(BF16)
    send_ref[...] = total[pl.ds(pl.multiple_of((1 - core) * half, half), half), :].astype(BF16)


def project(x_all, w_all):
    blocks, tokens, width = x_all.shape
    rows = w_all.shape[3]
    w_all = w_all.reshape(4, 2, 2, 4, rows, width)
    half = jax.ShapeDtypeStruct((tokens // 2, 8 * rows), BF16)
    return pl.pallas_call(
        project_kernel,
        grid=(8,),
        out_shape=(half, half),
        in_specs=[
            pl.BlockSpec(memory_space=pltpu.SMEM),
            pl.BlockSpec((blocks, tokens, width), lambda i: (0, 0, 0)),
            pl.BlockSpec((1, 2, 1, 4, rows, width), lambda i: (i % 4, 0, i // 4, 0, 0, 0)),
        ],
        out_specs=(pl.BlockSpec((tokens // 2, rows), lambda i: (0, i)),) * 2,
        scratch_shapes=[pltpu.VMEM((tokens, rows), F32)],
        compiler_params=pltpu.CompilerParams(dimension_semantics=("arbitrary",)),
        name="project",
    )(lax.axis_index(CORE).reshape(1).astype(jnp.int32), x_all, w_all)

def exactly(values, ones):
    high = values.astype(BF16)
    low = (values - high.astype(F32)).astype(BF16)
    ones = ones.astype(F32).astype(BF16)
    return nn(high, ones) + nn(low, ones)


def offset_of(turn):
    j = lax.rem(turn, 4)
    return lax.div(turn, 4), j + lax.div(j, 2) * (1 - 2 * lax.rem(j, 2))


FIRST_COLUMNS = 1792


def expert_kernel(
    keep_ref, other_ref, residual_ref, select_ref, gate_ref, bc_ref, w_hbm, saved_hbm,
    pre_hbm, route_ref, b_ref, c_ref,
    rows_out, held, w_ref, saved_buf, pre_buf, shares, part_out, part_in, sum_out, sum_in, bc_in, bc_sum, bc_other,
    w_sem, saved_sem, pre_sem, a_send, a_recv, g_send, g_recv, p_send, p_recv, q_send, q_recv, b_send, b_recv,
):
    turns, _, _, block, d = held.shape
    slots = block // 2
    hidden = w_ref.shape[0]
    seq = lax.axis_index("seq")
    x, y = lax.rem(seq, 4), lax.div(seq, 4)
    chip_y, chip_z, core = (lax.axis_index(name) for name in EXP)
    right = {"seq": y * 4 + lax.rem(x + 1, 4)}
    left = {"seq": y * 4 + lax.rem(x + 3, 4)}
    facing = {"seq": lax.rem(seq + 4, 8)}
    x_left, x_right, x_far = lax.rem(x + 3, 4), lax.rem(x + 1, 4), lax.rem(x + 2, 4)
    mates = [{"exp_2": 1 - core}]
    for turn in range(1, turns):
        by, bz = turn // 4, (0, 1, 3, 2)[turn % 4]
        for k in range(2):
            mates.append(
                {
                    "seq": lax.rem(seq + 4 * by, 8),
                    "exp_0": lax.rem(chip_y + by, 2),
                    "exp_1": lax.rem(chip_z + (4 - bz), 4),
                    "exp_2": k,
                }
            )
    mates += [{"seq": lax.rem(seq + k, 8)} for k in range(1, 8)]
    mates += [{"exp_0": 1 - chip_y, "exp_1": z, "exp_2": k} for z in range(4) for k in range(2)]
    barrier_with(mates)
    load_w = pltpu.make_async_copy(w_hbm.at[0], w_ref, w_sem.at[0])
    load_w.start()

    def chip_of(turn):
        by, bz = offset_of(turn)
        return lax.rem(chip_y + by, 2) * 4 + lax.rem(chip_z + bz, 4)

    def load_saved(turn):
        slot = lax.rem(turn, 2)
        return pltpu.make_async_copy(saved_hbm.at[:, chip_of(turn)], saved_buf.at[slot], saved_sem.at[slot])

    def store_pre(turn):
        slot = lax.rem(turn, 2)
        return pltpu.make_async_copy(pre_buf.at[slot], pre_hbm.at[:, chip_of(turn)], pre_sem.at[slot])

    load_saved(0).start()
    moe = (residual_ref[...].astype(F32) + keep_ref[...].astype(F32) + other_ref[...].astype(F32)).astype(BF16)
    rows = (nn(select_ref[...], moe) * gate_ref[...]).astype(BF16)
    rows_out[...] = rows.reshape(rows_out.shape)
    half_of = lambda c: pl.ds(pl.multiple_of(c * slots, slots), slots)

    def first_of(turn):
        return lax.rem(y + lax.div(turn, 4), 2)

    def to_expert(turn, k):
        by, bz = turn // 4, (0, 1, 3, 2)[turn % 4]
        ty, tz = lax.rem(chip_y + by, 2), lax.rem(chip_z + (4 - bz), 4)
        return pltpu.make_async_remote_copy(
            src_ref=rows_out.at[(ty * 4 + tz) * 2 + k],
            dst_ref=held.at[turn, y, x, half_of(core)],
            send_sem=a_send.at[turn, k],
            recv_sem=a_recv.at[turn, core],
            device_id={"seq": lax.rem(seq + 4 * by, 8), "exp_0": ty, "exp_1": tz, "exp_2": k},
            device_id_type=MESH,
        )

    def from_source(turn, c):
        there = held.at[turn, first_of(turn), x, half_of(c)]
        return pltpu.make_async_remote_copy(
            src_ref=there, dst_ref=there, send_sem=a_send.at[turn, 0], recv_sem=a_recv.at[turn, c],
            device_id={"exp_2": 1 - core}, device_id_type=MESH,
        )

    to_expert(0, 1 - core).start()
    for turn in range(1, turns):
        for k in range(2):
            to_expert(turn, k).start()
    held[0, y, x, half_of(core), :] = rows_out[(chip_y * 4 + chip_z) * 2 + core]

    first = pl.ds(0, FIRST_COLUMNS)
    rest = pl.ds(FIRST_COLUMNS, d - FIRST_COLUMNS)
    low, high, both = pl.ds(0, slots), pl.ds(slots, slots), slice(None)

    def moves(i, step):
        start = first_of(i)
        if step == 0:
            return (
                (0, held.at[i, start, x, both, first], held.at[i, start, x_left, both, first], right),
                (1, held.at[i, start, x, both, first], held.at[i, start, x_right, both, first], left),
                (2, held.at[i, start, x, both, rest], held.at[i, 1 - start, x, both, rest], facing),
            )
        if step == 1:
            return (
                (3, held.at[i, start, x_left, low, first], held.at[i, start, x_far, low, first], right),
                (4, held.at[i, start, x_right, high, first], held.at[i, start, x_far, high, first], left),
                (5, held.at[i, both, x, both, rest], held.at[i, both, x_left, both, rest], right),
                (6, held.at[i, both, x, both, rest], held.at[i, both, x_right, both, rest], left),
            )
        return (
            (7, held.at[i, start, both, both, first], held.at[i, 1 - start, both, both, first], facing),
            (8, held.at[i, both, x_left, low, rest], held.at[i, both, x_far, low, rest], right),
            (9, held.at[i, both, x_right, high, rest], held.at[i, both, x_far, high, rest], left),
        )

    def each(i, step, act):
        for number, sent, arriving, peer in moves(i, step):
            ref = arriving if act == "wait_recv" else sent
            copy = pltpu.make_async_remote_copy(
                src_ref=ref, dst_ref=ref, send_sem=g_send.at[i, number], recv_sem=g_recv.at[i, number],
                device_id=peer, device_id_type=MESH,
            )
            getattr(copy, act)()

    def compute(j):
        slot = lax.rem(j, 2)
        load_saved(j).wait()

        @pl.when(j < turns - 1)
        def _():
            load_saved(j + 1).start()

        @pl.when(j >= 2)
        def _():
            store_pre(j - 2).wait()

        count = 8 * block
        upstream = nt(held[j].reshape(count, d), w_ref[...])
        gate_pre = saved_buf[slot, :, :, 0, :].astype(F32).reshape(count, hidden)
        up_pre = saved_buf[slot, :, :, 1, :].astype(F32).reshape(count, hidden)
        sig = jax.nn.sigmoid(gate_pre)
        act = gate_pre * sig
        up_grad = upstream * act
        gate_grad = upstream * up_pre * sig * (1.0 + gate_pre * (1.0 - sig))
        pre_buf[slot, :, :, 0, :] = gate_grad.astype(BF16).reshape(8, block, hidden)
        pre_buf[slot, :, :, 1, :] = up_grad.astype(BF16).reshape(8, block, hidden)
        store_pre(j).start()
        sums = nt(jnp.ones((8, hidden), BF16), (up_grad * up_pre).astype(BF16))
        at = lambda dim, *shape: lax.broadcasted_iota(jnp.int32, shape, dim)
        sums = jnp.where(lax.div(at(1, 8, count), block) == at(0, 8, count), sums, 0.0)
        shares[...] += exactly(
            sums, lax.rem(at(0, count, turns * block), block) + chip_of(j) * block == at(1, count, turns * block)
        )

    column = chip_z * 2 + core

    def bc_copy(k, back=False):
        to, source = lax.rem(column + k, 8), lax.rem(column + (8 - k), 8)
        return pltpu.make_async_remote_copy(
            src_ref=bc_in.at[source] if back else bc_ref.at[:, to],
            dst_ref=bc_in.at[source] if back else bc_in.at[column],
            send_sem=b_send.at[k], recv_sem=b_recv.at[k],
            device_id={"exp_1": lax.div(to, 2), "exp_2": lax.rem(to, 2)}, device_id_type=MESH,
        )

    def bc_half():
        return pltpu.make_async_remote_copy(
            src_ref=bc_sum.at[1 - chip_y], dst_ref=bc_other, send_sem=b_send.at[0], recv_sem=b_recv.at[0],
            device_id={"exp_0": 1 - chip_y}, device_id_type=MESH,
        )

    def pass_on(t, carry):
        @pl.when(t == 3)
        def _():
            for k in range(1, 8):
                bc_copy(k).start()

        @pl.when(t == 6)
        def _():
            bc_in[column] = bc_ref[:, column]
            for k in range(1, 8):
                bc_copy(k, back=True).wait_recv()
            for half in range(2):
                summed = bc_in[0, half].astype(F32)
                for k in range(1, 8):
                    summed = summed + bc_in[k, half].astype(F32)
                bc_sum[half] = summed
            bc_half().start()

        @pl.when(t == 0)
        def _():
            from_source(0, 1 - core).wait_recv()
            each(0, 0, "start")

        @pl.when(jnp.logical_and(t >= 1, t < turns))
        def _():
            for c in range(2):
                from_source(t, c).wait_recv()
            each(t, 0, "start")

        @pl.when(jnp.logical_and(t >= 1, t < turns + 1))
        def _():
            each(t - 1, 0, "wait_recv")
            each(t - 1, 1, "start")

        @pl.when(jnp.logical_and(t >= 2, t < turns + 2))
        def _():
            each(t - 2, 1, "wait_recv")
            each(t - 2, 2, "start")

        @pl.when(t == 2)
        def _():
            load_w.wait()

        @pl.when(t >= 3)
        def _():
            each(t - 3, 2, "wait_recv")
            compute(t - 3)

        return carry

    shares[...] = jnp.zeros_like(shares)
    lax.fori_loop(0, turns + 3, pass_on, 0)
    all_exp = 16
    own = (chip_y * 4 + chip_z) * 2 + core

    def exp_device(index):
        return {"exp_0": lax.div(index, 8), "exp_1": lax.rem(lax.div(index, 2), 4), "exp_2": lax.rem(index, 2)}

    def part(k, back=False):
        to, source = lax.rem(seq + k, 8), lax.rem(seq + (8 - k), 8)
        return pltpu.make_async_remote_copy(
            src_ref=part_in.at[source] if back else part_out.at[to],
            dst_ref=part_in.at[source] if back else part_in.at[seq],
            send_sem=p_send.at[k - 1], recv_sem=p_recv.at[k - 1], device_id={"seq": to}, device_id_type=MESH,
        )

    def total(k, back=False):
        to, source = lax.rem(own + k, all_exp), lax.rem(own + (all_exp - k), all_exp)
        return pltpu.make_async_remote_copy(
            src_ref=sum_in.at[source] if back else sum_out.at[to],
            dst_ref=sum_in.at[source] if back else sum_in.at[own],
            send_sem=q_send.at[k - 1], recv_sem=q_recv.at[k - 1], device_id=exp_device(to), device_id_type=MESH,
        )

    for k in range(8):
        part_out[k] = shares[k : k + 1, :]
    for k in range(1, 8):
        part(k).start()
    part_in[seq] = part_out[seq]
    for k in range(1, 8):
        part(k, back=True).wait_recv()
    summed = part_in[0]
    for k in range(1, 8):
        summed = summed + part_in[k]
    at = lambda dim, *shape: lax.broadcasted_iota(jnp.int32, shape, dim)
    width = summed.shape[1]
    each_exp = jnp.where(lax.div(at(1, all_exp, width), slots) == at(0, all_exp, width), summed, 0.0)
    each_exp = exactly(each_exp, lax.rem(at(0, width, 128), slots) == at(1, width, 128))
    for k in range(all_exp):
        sum_out[k] = each_exp[k : k + 1, :]
    for k in range(1, all_exp):
        total(k).start()
    sum_in[own] = sum_out[own]
    for k in range(1, all_exp):
        total(k, back=True).wait_recv()
    for k in range(all_exp):
        route_ref[k : k + 1, :] = sum_in[k]
    for k in range(1, 8):
        part(k).wait_send()
    for k in range(1, all_exp):
        total(k).wait_send()
    bc_half().wait_recv()
    summed = bc_sum[chip_y] + bc_other[...]
    b_ref[...] = summed[:, :128]
    c_ref[...] = summed[:, 128:]
    bc_half().wait_send()
    for k in range(1, 8):
        bc_copy(k).wait_send()
    store_pre(turns - 2).wait()
    store_pre(turns - 1).wait()
    to_expert(0, 1 - core).wait_send()
    for turn in range(1, turns):
        for k in range(2):
            to_expert(turn, k).wait_send()

    def sent(i, carry):
        for step in range(3):
            each(i, step, "wait_send")
        return carry

    lax.fori_loop(0, turns, sent, 0)


def expert_part(keep, other, residual, select, slot_gates, bc_grads, w_down, saved_pre):
    slots, _, hidden = saved_pre.shape[1:]
    d = residual.shape[1]
    rows = select.shape[0]
    turns, block = 8, rows // 8
    vmem = pl.BlockSpec(memory_space=pltpu.VMEM)
    hbm = pl.BlockSpec(memory_space=pl.ANY)
    dma = pltpu.SemaphoreType.DMA
    tokens = residual.shape[0]
    bc_grads = bc_grads.reshape(2, 8, tokens, 256)
    pre, route, b_grads, c_grads = pl.pallas_call(
        expert_kernel,
        out_shape=(
            jax.ShapeDtypeStruct((8, turns, block, 2, hidden), BF16),
            jax.ShapeDtypeStruct((16, 128), F32),
            jax.ShapeDtypeStruct((tokens, 128), F32),
            jax.ShapeDtypeStruct((tokens, 128), F32),
        ),
        in_specs=[vmem] * 6 + [hbm] * 2,
        out_specs=(hbm, vmem, vmem, vmem),
        scratch_shapes=[
            pltpu.VMEM((16, rows // 16, d), BF16),
            pltpu.VMEM((turns, 2, 4, block, d), BF16),
            pltpu.VMEM((hidden, d), BF16),
            pltpu.VMEM((2, 8, block, 2, hidden), BF16),
            pltpu.VMEM((2, 8, block, 2, hidden), BF16),
            pltpu.VMEM((8, turns * block), F32),
            pltpu.VMEM((8, 1, turns * block), F32),
            pltpu.VMEM((8, 1, turns * block), F32),
            pltpu.VMEM((16, 1, 128), F32),
            pltpu.VMEM((16, 1, 128), F32),
            pltpu.VMEM((8, 2, tokens, 256), BF16),
            pltpu.VMEM((2, tokens, 256), F32),
            pltpu.VMEM((tokens, 256), F32),
            dma((1,)),
            dma((2,)),
            dma((2,)),
            dma((turns, 2)),
            dma((turns, 2)),
            dma((turns, 10)),
            dma((turns, 10)),
            dma((7,)),
            dma((7,)),
            dma((15,)),
            dma((15,)),
            dma((8,)),
            dma((8,)),
        ],
        compiler_params=pltpu.CompilerParams(
            collective_id=2, has_side_effects=True, vmem_limit_bytes=60 * 2**20
        ),
        name="experts",
    )(keep, other, residual, select, slot_gates, bc_grads, w_down, saved_pre.reshape(8, turns, block, 2, hidden))
    return pre.reshape(saved_pre.shape), route[:, : block // 2].reshape(-1), b_grads, c_grads


def per_device(
    gates, expert_ids, saved_pre, w_down, residual_grad, in_weight, ssm_in, b_proj, c_proj, step_sizes, a_log, skip_gain, ssm_grad
):
    w_all, x_all, bc_grads, step_grads = ssm_part(
        in_weight, ssm_in, b_proj, c_proj, step_sizes, a_log, skip_gain, ssm_grad
    )
    tokens_here = residual_grad.shape[0]
    experts = lax.axis_size(EXP)
    capacity = TOPK * tokens_here // experts
    keep, send = project(x_all, w_all)
    other = lax.ppermute(send, CORE, [(0, 1), (1, 0)])
    flat_ids = expert_ids.reshape(-1)
    onehot = (flat_ids[:, None] == jnp.arange(experts, dtype=jnp.int32)[None, :]).astype(jnp.int32)
    position = jnp.sum(onehot * jnp.cumsum(onehot, axis=0), axis=1) - 1
    target = flat_ids * capacity + position
    selector = target[:, None] == jnp.arange(experts * capacity, dtype=jnp.int32)[None, :]
    by_token = selector.reshape(tokens_here, TOPK, -1)
    slot_gates = jnp.sum(by_token * gates[:, :, None], axis=(0, 1))
    select = jnp.any(by_token, axis=1).astype(BF16).T
    pre_grads, totals, b_grads, c_grads = expert_part(
        keep, other, residual_grad, select, slot_gates[:, None], bc_grads, w_down, saved_pre
    )
    route_grads = totals[target].reshape(tokens_here, TOPK) / gates
    return (pre_grads, route_grads, b_grads, c_grads, step_grads)


def solution(mesh):
    split = Mesh(mesh.devices.reshape(mesh.shape["seq"], 2, 4, 2), ("seq", "exp_0", "exp_1", "exp_2"))
    in_specs = (
        P(SEQ_EXP, None), P(SEQ_EXP, None), P(EXP, None, None, "seq"), P(EXP, "seq", None), P(SEQ_EXP, None), P("seq", EXP),
        P("seq", EXP), P("seq", None), P("seq", None), P(EXP, "seq"), P(EXP), P(EXP), P("seq", EXP),
    )
    out_specs = (P(EXP, None, None, "seq"), P(SEQ_EXP, None), P(SEQ_EXP, None), P(SEQ_EXP, None), P(EXP, "seq"))
    return jax.shard_map(per_device, mesh=split, in_specs=in_specs, out_specs=out_specs, check_vma=False)
```

```python
import functools

import jax
import jax.numpy as jnp
from jax import lax
from jax.experimental import pallas as pl
from jax.experimental.pallas import tpu as pltpu
from jax.sharding import Mesh
from jax.sharding import PartitionSpec as P

TOPK = 2
HDIM = 64
SPAN = 256
CHIPS = ("exp_0", "exp_1")
CORE = "exp_2"
EXP = ("exp_0", "exp_1", "exp_2")
SEQ_EXP = ("seq", "exp_0", "exp_1", "exp_2")
F32 = jnp.float32
BF16 = jnp.bfloat16
MESH = pl.DeviceIdType.MESH


def nn(a, b):
    return lax.dot_general(a, b, (((1,), (0,)), ((), ())), preferred_element_type=F32)


def nt(a, b):
    return lax.dot_general(a, b, (((1,), (1,)), ((), ())), preferred_element_type=F32)


def tn(a, b):
    return lax.dot_general(a, b, (((0,), (0,)), ((), ())), preferred_element_type=F32)


def over_lanes(columns):
    rows, heads = columns.shape
    lane = lax.broadcasted_iota(jnp.int32, (rows, 2 * HDIM), 1)
    return jnp.concatenate(
        [
            jnp.where(lane < HDIM, columns[:, h : h + 1], columns[:, h + 1 : h + 2])
            for h in range(0, heads, 2)
        ],
        axis=1,
    )


def decays(lcol_ref):
    running = lcol_ref[...]
    last = running[SPAN - 1 : SPAN, :]
    return over_lanes(jnp.exp(-running)), over_lanes(jnp.exp(running - last))


def barrier_with(peers):
    semaphore = pltpu.get_barrier_semaphore()
    for peer in peers:
        pl.semaphore_signal(semaphore, inc=1, device_id=peer, device_id_type=MESH)
    pl.semaphore_wait(semaphore, len(peers))


ORDERS = ("xyz", "yzx", "zxy", "xzy", "yxz", "zyx")
SHARES = (5, 6, 5, 5, 5, 6)
UNIT = 16


class Torus:
    def __init__(self):
        seq = lax.axis_index("seq")
        self.at = {
            "x": lax.rem(seq, 4),
            "y": lax.axis_index("exp_0") * 2 + lax.div(seq, 4),
            "z": lax.axis_index("exp_1"),
        }

    def device(self, dim, step):
        at = dict(self.at)
        at[dim] = lax.rem(at[dim] + (step + 4), 4)
        return {"seq": lax.rem(at["y"], 2) * 4 + at["x"], "exp_0": lax.div(at["y"], 2), "exp_1": at["z"]}


class Gather:
    def __init__(self, torus, own_ref, out_ref, send_sem, recv_sem):
        self.torus, self.own, self.out = torus, own_ref, out_ref
        self.send_sem, self.recv_sem = send_sem, recv_sem
        self.rows = [(sum(SHARES[:k]) * UNIT, SHARES[k] * UNIT) for k in range(len(ORDERS))]

    def block(self, stream, phase, step, start, size):
        order = ORDERS[stream]
        at = []
        for dim in "xyz":
            k = order.index(dim)
            if k < phase:
                at.append(slice(None))
            elif k == phase:
                at.append(lax.rem(self.torus.at[dim] + (step + 4), 4))
            else:
                at.append(self.torus.at[dim])
        return self.out.at[(*at, pl.ds(start, size), slice(None))]

    def copies(self, stream, step, back=False):
        phase, second = step // 2, step % 2
        dim = ORDERS[stream][phase]
        start, size = self.rows[stream]
        half = (size // UNIT + 1) // 2 * UNIT
        made = []
        for side, way in enumerate((1, -1)):
            if not second:
                span, hop = (start, size), 0
            else:
                span = (start, half) if side == 0 else (start + half, size - half)
                hop = -way
            sent = self.block(stream, phase, hop, *span)
            here = sent
            if step == 0:
                sent = self.own.at[pl.ds(*span), :]
            common = dict(
                send_sem=self.send_sem.at[stream, step, side],
                recv_sem=self.recv_sem.at[stream, step, side],
                device_id=self.torus.device(dim, way),
                device_id_type=MESH,
            )
            if back:
                sent = here = self.block(stream, phase, hop - way, *span)
            made.append(pltpu.make_async_remote_copy(src_ref=sent, dst_ref=here, **common))
        return made

    def start(self, stream, step):
        for copy in self.copies(stream, step):
            copy.start()

    def arrived(self, stream, step):
        for copy in self.copies(stream, step, back=True):
            copy.wait_recv()

    def advance(self, step, streams):
        for stream in streams:
            if step > 0:
                self.arrived(stream, step - 1)
            if step < 6:
                self.start(stream, step)

    def drain(self):
        for stream in range(len(ORDERS)):
            for step in range(6):
                for copy in self.copies(stream, step):
                    copy.wait_send()


def ssm_kernel(
    w_hbm, x_hbm, g_hbm, b_hbm, c_hbm, step_hbm, a_ref, skip_ref,
    all_ref, dx_ref, dbc_ref, dq_ref,
    w_ref, x_ref, g_ref, b_ref, c_ref, step_ref, lcol_ref, lrow_ref, whole_ref, before_ref, s_all, g_all, s_acc, g_acc, ends, got, dx_all,
    load_sem, own_sem, w_send, w_recv, s_send, s_recv, x_send, x_recv,
):
    chunks = s_all.shape[0]
    parts = got.shape[0]
    width = x_ref.shape[1]
    heads = width // HDIM
    torus = Torus()
    me = lax.axis_index("seq")
    place = lax.axis_index("exp_0") * 4 + lax.axis_index("exp_1")

    def in_part(offset):
        return lax.rem(me + offset, parts)

    def chip_at(index):
        return {"exp_0": lax.div(index, 4), "exp_1": lax.rem(index, 4)}

    pairs_in = ((w_hbm, w_ref), (x_hbm, x_ref), (g_hbm, g_ref), (b_hbm, b_ref), (c_hbm, c_ref), (step_hbm, step_ref))
    loads = [pltpu.make_async_copy(a, b, load_sem.at[k]) for k, (a, b) in enumerate(pairs_in)]
    for load in loads:
        load.start()
    across_y = {"seq": lax.rem(me + 4, 8), "exp_0": 1 - lax.axis_index("exp_0")}
    barrier_with(
        [{"seq": in_part(o)} for o in range(1, parts)]
        + [chip_at(lax.rem(place + o, chunks)) for o in range(1, chunks)]
        + [across_y]
    )
    gather = Gather(torus, w_ref, all_ref, w_send, w_recv)
    streams = range(len(ORDERS))
    loads[0].wait()
    gather.advance(0, streams)
    here = torus.at
    own = pltpu.make_async_copy(w_ref, all_ref.at[here["x"], here["y"], here["z"]], own_sem.at[0])
    own.start()

    def rows_of(chunk):
        return pl.ds(pl.multiple_of(chunk * SPAN, SPAN), SPAN)

    s_acc[...] = jnp.zeros_like(s_acc)
    g_acc[...] = jnp.zeros_like(g_acc)

    def states(chunk, carry):
        @pl.when(chunk == 3)
        def _():
            gather.advance(1, streams)

        rows = rows_of(chunk)
        from_start, to_end = decays(lcol_ref.at[rows])
        fresh = tn(b_ref[rows, :], (x_ref[rows, :].astype(F32) * to_end).astype(BF16))
        back = tn(c_ref[rows, :], (g_ref[rows, :].astype(F32) * from_start).astype(BF16))
        s_all[chunk] = fresh
        g_all[chunk] = back
        s_acc[...] = s_acc[...] * whole_ref[chunk] + fresh
        g_acc[...] = g_acc[...] + before_ref[chunk] * back
        return carry

    for load in loads[1:]:
        load.wait()
    row = lax.broadcasted_iota(jnp.int32, (SPAN, SPAN), 0)
    col = lax.broadcasted_iota(jnp.int32, (SPAN, SPAN), 1)
    rates = [jnp.exp(jnp.full((1, SPAN), a_ref[h], F32)) for h in range(heads)]
    rate_rows = jnp.concatenate(rates, axis=0)
    steps = jnp.concatenate([step_ref[:, k * SPAN : (k + 1) * SPAN] * rate_rows for k in range(chunks)], axis=0)
    until = (row <= col).astype(F32).astype(BF16)
    high = steps.astype(BF16)
    rest = steps - high.astype(F32)
    middle = rest.astype(BF16)
    low = (rest - middle.astype(F32)).astype(BF16)
    running = nn(high, until) + nn(middle, until) + nn(low, until)
    columns = running.T
    passed = jnp.zeros((1, heads), F32)
    for k in range(chunks):
        lrow_ref[:, k * SPAN : (k + 1) * SPAN] = running[k * heads : (k + 1) * heads, :]
        mine = columns[:, k * heads : (k + 1) * heads]
        lcol_ref[k * SPAN : (k + 1) * SPAN, :] = mine
        last = mine[SPAN - 1 : SPAN, :]
        whole_ref[k] = over_lanes(jnp.exp(-last))
        before_ref[k] = over_lanes(jnp.exp(-passed))
        passed = passed + last
    part_decay = over_lanes(jnp.exp(-passed))
    high = part_decay.astype(BF16).astype(F32)
    line = lax.broadcasted_iota(jnp.int32, (16, width), 0)
    tail = jnp.where(line == 0, high, jnp.where(line == 1, part_decay - high, 0.0)).astype(BF16)
    lane_head = lax.broadcasted_iota(jnp.int32, (1, width), 1) // HDIM
    skip = jnp.zeros((1, width), F32)
    for h in range(heads):
        skip = jnp.where(lane_head == h, skip_ref[h], skip)
    lax.fori_loop(0, chunks, states, 0)
    ends[0, :128, :] = s_acc[...].astype(BF16)
    ends[1, :128, :] = g_acc[...].astype(BF16)
    ends[0, 128:, :] = tail
    ends[1, 128:, :] = tail

    def to_part(offset, back=False):
        peer = in_part(offset)
        source = in_part(parts - offset)
        common = dict(
            send_sem=s_send.at[offset - 1], recv_sem=s_recv.at[offset - 1], device_id={"seq": peer}, device_id_type=MESH
        )
        which = jnp.where(peer > me, 0, 1)
        if back:
            return pltpu.make_async_remote_copy(src_ref=got.at[source], dst_ref=got.at[source], **common)
        return pltpu.make_async_remote_copy(src_ref=ends.at[which], dst_ref=got.at[me], **common)

    for offset in range(1, parts):
        to_part(offset).start()
    own.wait()
    gather.advance(2, streams)
    got[me] = jnp.zeros(got.shape[1:], BF16)
    for offset in range(1, parts):
        to_part(offset, back=True).wait_recv()

    def decay_of(m):
        return got[m, 128:129, :].astype(F32) + got[m, 129:130, :].astype(F32)

    state = jnp.zeros((128, width), F32)
    for m in range(parts):
        state = jnp.where(m < me, decay_of(m) * state + got[m, :128, :].astype(F32), state)
    for k in range(chunks):
        fresh = s_all[k]
        s_all[k] = state
        state = state * whole_ref[k] + fresh
    state = jnp.zeros((128, width), F32)
    for m in reversed(range(parts)):
        state = jnp.where(m > me, decay_of(m) * state + got[m, :128, :].astype(F32), state)
    for k in reversed(range(chunks)):
        fresh = g_all[k]
        g_all[k] = state
        state = state * whole_ref[k] + fresh

    head_of = lax.broadcasted_iota(jnp.int32, (8, width), 1) // HDIM
    pick = (head_of == lax.broadcasted_iota(jnp.int32, (8, width), 0)).astype(F32)
    pick_half = pick.astype(BF16)

    def to_chip(turn, back=False):
        target = lax.rem(place + 1 + turn, chunks)
        source = lax.rem(place + (chunks - 1) - turn, chunks)
        common = dict(
            send_sem=x_send.at[turn], recv_sem=x_recv.at[turn], device_id=chip_at(target), device_id_type=MESH
        )
        if back:
            return pltpu.make_async_remote_copy(src_ref=dx_ref.at[source], dst_ref=dx_ref.at[source], **common)
        return pltpu.make_async_remote_copy(src_ref=dx_all.at[target], dst_ref=dx_ref.at[place], **common)

    def grads(turn, carry):
        chunk = lax.rem(place + 1 + turn, chunks)
        rows = rows_of(chunk)
        x = x_ref[rows, :]
        g = g_ref[rows, :]
        b = b_ref[rows, :]
        c = c_ref[rows, :]
        lcol = lcol_ref[rows, :]
        lrow = lrow_ref[:, rows]
        s_in = s_all[chunk]
        g_out = g_all[chunk]
        s_half = s_in.astype(BF16)
        g_half = g_out.astype(BF16)
        upper = row <= col
        strict = row < col
        from_row = (row >= col).astype(F32).astype(BF16)
        before_row = strict.astype(F32).astype(BF16)
        bc = nt(b, c)
        dx = jnp.zeros((SPAN, width), F32)
        pairs = jnp.zeros((SPAN, SPAN), F32)
        inside = []
        for h in range(heads):
            mine = pick_half[h : h + 1, :]
            m = nt(x * mine, g)
            w = jnp.exp(jnp.where(upper, lcol[:, h : h + 1] - lrow[h : h + 1, :], -1e30))
            a1 = w * bc
            pairs = pairs + w * m
            dx = dx + nn(a1.astype(BF16), g * mine)
            p = jnp.where(strict, a1 * m, 0.0).astype(BF16)
            inside.append(jnp.sum(jnp.where(strict, nn(p, from_row), 0.0), axis=0, keepdims=True))
        from_start, to_end = decays(lcol_ref.at[rows])
        ge = (g.astype(F32) * from_start).astype(BF16)
        xe = (x.astype(F32) * to_end).astype(BF16)
        pairs_half = pairs.astype(BF16)
        z = nn(c, s_half)
        v = nn(b, g_half)
        dbc_ref[rows, :128] = (nn(pairs_half, c) + nt(xe, g_half)).astype(BF16)
        dbc_ref[rows, 128:] = (tn(pairs_half, b) + nt(ge, s_half)).astype(BF16)
        dx_all[chunk] = (dx + to_end * v + skip * g.astype(F32)).astype(BF16)

        @pl.when(turn < chunks - 1)
        def _():
            to_chip(turn).start()

        rc = nt(pick_half, (ge.astype(F32) * z).astype(BF16))
        cc = nt(pick_half, (xe.astype(F32) * v).astype(BF16))
        across = jnp.sum(s_in * g_out, axis=0, keepdims=True) * whole_ref[chunk]
        ones = jnp.ones((width, SPAN), BF16)
        dq = nn(rc.astype(BF16), from_row) + nn(cc.astype(BF16), before_row) + nn((pick * across).astype(BF16), ones)
        for h in range(heads):
            dq_ref[h : h + 1, rows] = -(dq[h : h + 1, :] + inside[h]) * rates[h]
        for step, after in STEPS_AFTER:

            @pl.when(turn == after)
            def _(step=step):
                gather.advance(step, streams)

        return carry

    lax.fori_loop(0, chunks, grads, 0)
    mine = pltpu.make_async_copy(dx_all.at[place], dx_ref.at[place], own_sem.at[0])
    mine.start()
    for step in LAST_STEPS:
        gather.advance(step, streams)
    mine.wait()
    for turn in range(chunks - 1):
        to_chip(turn, back=True).wait_recv()
        to_chip(turn).wait_send()
    for offset in range(1, parts):
        to_part(offset).wait_send()
    gather.drain()


STEPS_AFTER = ((3, 0), (4, 3))
LAST_STEPS = (5, 6)


def ssm_part(in_weight, ssm_in, b_proj, c_proj, step_sizes, a_log, skip_gain, ssm_grad):
    length, width = ssm_in.shape
    heads = width // HDIM
    chunks = length // SPAN
    parts = lax.axis_size("seq")
    vmem = pl.BlockSpec(memory_space=pltpu.VMEM)
    hbm = pl.BlockSpec(memory_space=pl.ANY)
    streams = len(ORDERS)
    dma = pltpu.SemaphoreType.DMA
    return pl.pallas_call(
        ssm_kernel,
        out_shape=(
            jax.ShapeDtypeStruct((4, 4, 4, *in_weight.shape), BF16),
            jax.ShapeDtypeStruct((chunks, SPAN, width), BF16),
            jax.ShapeDtypeStruct((length, 256), BF16),
            jax.ShapeDtypeStruct((heads, length), F32),
        ),
        in_specs=[pl.BlockSpec(memory_space=pltpu.HBM)] * 6 + [pl.BlockSpec(memory_space=pltpu.SMEM)] * 2,
        out_specs=(hbm, hbm, vmem, vmem),
        scratch_shapes=[
            pltpu.VMEM(in_weight.shape, BF16),
            pltpu.VMEM((length, width), BF16),
            pltpu.VMEM((length, width), BF16),
            pltpu.VMEM((length, 128), BF16),
            pltpu.VMEM((length, 128), BF16),
            pltpu.VMEM((heads, length), F32),
            pltpu.VMEM((length, heads), F32),
            pltpu.VMEM((heads, length), F32),
            pltpu.VMEM((chunks, 1, width), F32),
            pltpu.VMEM((chunks, 1, width), F32),
            pltpu.VMEM((chunks, 128, width), F32),
            pltpu.VMEM((chunks, 128, width), F32),
            pltpu.VMEM((128, width), F32),
            pltpu.VMEM((128, width), F32),
            pltpu.VMEM((2, 144, width), BF16),
            pltpu.VMEM((parts, 144, width), BF16),
            pltpu.VMEM((chunks, SPAN, width), BF16),
            dma((6,)),
            dma((1,)),
            dma((streams, 6, 2)),
            dma((streams, 6, 2)),
            dma((parts - 1,)),
            dma((parts - 1,)),
            dma((chunks - 1,)),
            dma((chunks - 1,)),
        ],
        compiler_params=pltpu.CompilerParams(
            collective_id=1, has_side_effects=True, vmem_limit_bytes=63 * 2**20
        ),
        name="ssm",
    )(in_weight, ssm_in, ssm_grad, b_proj, c_proj, step_sizes, a_log, skip_gain)


def project_kernel(core_ref, x_ref, w_hbm, keep_ref, send_ref, w_ref, total, sem):
    core = core_ref[0]
    half = keep_ref.shape[0]
    rows = w_ref.shape[3]
    blocks = w_ref.shape[0]

    def load(i):
        return pltpu.make_async_copy(w_hbm.at[i % 4, :, i // 4], w_ref.at[i], sem.at[i])

    for i in range(blocks):
        load(i).start()
    for i in range(blocks):
        load(i).wait()
        acc = jnp.zeros(total.shape, F32)
        for k in range(x_ref.shape[0]):
            acc = acc + nt(x_ref[k], w_ref[i, k // 4, k % 4])
        total[...] = acc
        columns = slice(i * rows, (i + 1) * rows)
        keep_ref[:, columns] = total[pl.ds(pl.multiple_of(core * half, half), half), :].astype(BF16)
        send_ref[:, columns] = total[pl.ds(pl.multiple_of((1 - core) * half, half), half), :].astype(BF16)


def project(x_all, w_all):
    blocks, tokens, width = x_all.shape
    rows = w_all.shape[3]
    w_all = w_all.reshape(4, 2, 2, 4, rows, width)
    half = jax.ShapeDtypeStruct((tokens // 2, 8 * rows), BF16)
    vmem = pl.BlockSpec(memory_space=pltpu.VMEM)
    return pl.pallas_call(
        project_kernel,
        out_shape=(half, half),
        in_specs=[pl.BlockSpec(memory_space=pltpu.SMEM), vmem, pl.BlockSpec(memory_space=pltpu.HBM)],
        out_specs=(vmem, vmem),
        scratch_shapes=[
            pltpu.VMEM((8, 2, 4, rows, width), BF16),
            pltpu.VMEM((tokens, rows), F32),
            pltpu.SemaphoreType.DMA((8,)),
        ],
        compiler_params=pltpu.CompilerParams(vmem_limit_bytes=48 * 2**20),
        name="project",
    )(lax.axis_index(CORE).reshape(1).astype(jnp.int32), x_all, w_all)


def exactly(values, ones):
    high = values.astype(BF16)
    low = (values - high.astype(F32)).astype(BF16)
    ones = ones.astype(F32).astype(BF16)
    return nn(high, ones) + nn(low, ones)


def offset_of(turn):
    j = lax.rem(turn, 4)
    return lax.div(turn, 4), j + lax.div(j, 2) * (1 - 2 * lax.rem(j, 2))


FIRST_COLUMNS = 1792


def expert_kernel(
    keep_ref, other_ref, residual_ref, select_ref, gate_ref, bc_ref, w_hbm, saved_hbm,
    pre_hbm, route_ref, b_ref, c_ref,
    rows_out, held, w_ref, saved_buf, pre_buf, shares, part_out, part_in, sum_out, sum_in, bc_in, bc_sum, bc_other,
    w_sem, saved_sem, pre_sem, a_send, a_recv, g_send, g_recv, p_send, p_recv, q_send, q_recv, b_send, b_recv,
):
    turns, _, _, block, d = held.shape
    slots = block // 2
    hidden = w_ref.shape[0]
    seq = lax.axis_index("seq")
    x, y = lax.rem(seq, 4), lax.div(seq, 4)
    chip_y, chip_z, core = (lax.axis_index(name) for name in EXP)
    right = {"seq": y * 4 + lax.rem(x + 1, 4)}
    left = {"seq": y * 4 + lax.rem(x + 3, 4)}
    facing = {"seq": lax.rem(seq + 4, 8)}
    x_left, x_right, x_far = lax.rem(x + 3, 4), lax.rem(x + 1, 4), lax.rem(x + 2, 4)
    mates = [{"exp_2": 1 - core}]
    for turn in range(1, turns):
        by, bz = turn // 4, (0, 1, 3, 2)[turn % 4]
        for k in range(2):
            mates.append(
                {
                    "seq": lax.rem(seq + 4 * by, 8),
                    "exp_0": lax.rem(chip_y + by, 2),
                    "exp_1": lax.rem(chip_z + (4 - bz), 4),
                    "exp_2": k,
                }
            )
    mates += [{"seq": lax.rem(seq + k, 8)} for k in range(1, 8)]
    mates += [{"exp_0": 1 - chip_y, "exp_1": z, "exp_2": k} for z in range(4) for k in range(2)]
    barrier_with(mates)
    load_w = pltpu.make_async_copy(w_hbm.at[0], w_ref, w_sem.at[0])
    load_w.start()

    def chip_of(turn):
        by, bz = offset_of(turn)
        return lax.rem(chip_y + by, 2) * 4 + lax.rem(chip_z + bz, 4)

    def load_saved(turn):
        slot = lax.rem(turn, 2)
        return pltpu.make_async_copy(saved_hbm.at[:, chip_of(turn)], saved_buf.at[slot], saved_sem.at[slot])

    def store_pre(turn):
        slot = lax.rem(turn, 2)
        return pltpu.make_async_copy(pre_buf.at[slot], pre_hbm.at[:, chip_of(turn)], pre_sem.at[slot])

    load_saved(0).start()
    moe = (residual_ref[...].astype(F32) + keep_ref[...].astype(F32) + other_ref[...].astype(F32)).astype(BF16)
    rows = (nn(select_ref[...], moe) * gate_ref[...]).astype(BF16)
    rows_out[...] = rows.reshape(rows_out.shape)
    half_of = lambda c: pl.ds(pl.multiple_of(c * slots, slots), slots)

    def first_of(turn):
        return lax.rem(y + lax.div(turn, 4), 2)

    def to_expert(turn, k):
        by, bz = turn // 4, (0, 1, 3, 2)[turn % 4]
        ty, tz = lax.rem(chip_y + by, 2), lax.rem(chip_z + (4 - bz), 4)
        return pltpu.make_async_remote_copy(
            src_ref=rows_out.at[(ty * 4 + tz) * 2 + k],
            dst_ref=held.at[turn, y, x, half_of(core)],
            send_sem=a_send.at[turn, k],
            recv_sem=a_recv.at[turn, core],
            device_id={"seq": lax.rem(seq + 4 * by, 8), "exp_0": ty, "exp_1": tz, "exp_2": k},
            device_id_type=MESH,
        )

    def from_source(turn, c):
        there = held.at[turn, first_of(turn), x, half_of(c)]
        return pltpu.make_async_remote_copy(
            src_ref=there, dst_ref=there, send_sem=a_send.at[turn, 0], recv_sem=a_recv.at[turn, c],
            device_id={"exp_2": 1 - core}, device_id_type=MESH,
        )

    to_expert(0, 1 - core).start()
    for turn in range(1, turns):
        for k in range(2):
            to_expert(turn, k).start()
    held[0, y, x, half_of(core), :] = rows_out[(chip_y * 4 + chip_z) * 2 + core]

    first = pl.ds(0, FIRST_COLUMNS)
    rest = pl.ds(FIRST_COLUMNS, d - FIRST_COLUMNS)
    low, high, both = pl.ds(0, slots), pl.ds(slots, slots), slice(None)

    def moves(i, step):
        start = first_of(i)
        if step == 0:
            return (
                (0, held.at[i, start, x, both, first], held.at[i, start, x_left, both, first], right),
                (1, held.at[i, start, x, both, first], held.at[i, start, x_right, both, first], left),
                (2, held.at[i, start, x, both, rest], held.at[i, 1 - start, x, both, rest], facing),
            )
        if step == 1:
            return (
                (3, held.at[i, start, x_left, low, first], held.at[i, start, x_far, low, first], right),
                (4, held.at[i, start, x_right, high, first], held.at[i, start, x_far, high, first], left),
                (5, held.at[i, both, x, both, rest], held.at[i, both, x_left, both, rest], right),
                (6, held.at[i, both, x, both, rest], held.at[i, both, x_right, both, rest], left),
            )
        return (
            (7, held.at[i, start, both, both, first], held.at[i, 1 - start, both, both, first], facing),
            (8, held.at[i, both, x_left, low, rest], held.at[i, both, x_far, low, rest], right),
            (9, held.at[i, both, x_right, high, rest], held.at[i, both, x_far, high, rest], left),
        )

    def each(i, step, act):
        for number, sent, arriving, peer in moves(i, step):
            ref = arriving if act == "wait_recv" else sent
            copy = pltpu.make_async_remote_copy(
                src_ref=ref, dst_ref=ref, send_sem=g_send.at[i, number], recv_sem=g_recv.at[i, number],
                device_id=peer, device_id_type=MESH,
            )
            getattr(copy, act)()

    def compute(j):
        slot = lax.rem(j, 2)
        load_saved(j).wait()

        @pl.when(j < turns - 1)
        def _():
            load_saved(j + 1).start()

        @pl.when(j >= 2)
        def _():
            store_pre(j - 2).wait()

        count = 8 * block
        upstream = nt(held[j].reshape(count, d), w_ref[...])
        gate_pre = saved_buf[slot, :, :, 0, :].astype(F32).reshape(count, hidden)
        up_pre = saved_buf[slot, :, :, 1, :].astype(F32).reshape(count, hidden)
        sig = jax.nn.sigmoid(gate_pre)
        act = gate_pre * sig
        up_grad = upstream * act
        gate_grad = upstream * up_pre * sig * (1.0 + gate_pre * (1.0 - sig))
        pre_buf[slot, :, :, 0, :] = gate_grad.astype(BF16).reshape(8, block, hidden)
        pre_buf[slot, :, :, 1, :] = up_grad.astype(BF16).reshape(8, block, hidden)
        store_pre(j).start()
        sums = nt(jnp.ones((8, hidden), BF16), (up_grad * up_pre).astype(BF16))
        at = lambda dim, *shape: lax.broadcasted_iota(jnp.int32, shape, dim)
        sums = jnp.where(lax.div(at(1, 8, count), block) == at(0, 8, count), sums, 0.0)
        shares[...] += exactly(
            sums, lax.rem(at(0, count, turns * block), block) + chip_of(j) * block == at(1, count, turns * block)
        )

    column = chip_z * 2 + core

    def bc_copy(k, back=False):
        to, source = lax.rem(column + k, 8), lax.rem(column + (8 - k), 8)
        return pltpu.make_async_remote_copy(
            src_ref=bc_in.at[source] if back else bc_ref.at[:, to],
            dst_ref=bc_in.at[source] if back else bc_in.at[column],
            send_sem=b_send.at[k], recv_sem=b_recv.at[k],
            device_id={"exp_1": lax.div(to, 2), "exp_2": lax.rem(to, 2)}, device_id_type=MESH,
        )

    def bc_half():
        return pltpu.make_async_remote_copy(
            src_ref=bc_sum.at[1 - chip_y], dst_ref=bc_other, send_sem=b_send.at[0], recv_sem=b_recv.at[0],
            device_id={"exp_0": 1 - chip_y}, device_id_type=MESH,
        )

    def pass_on(t, carry):
        @pl.when(t == 3)
        def _():
            for k in range(1, 8):
                bc_copy(k).start()

        @pl.when(t == 6)
        def _():
            bc_in[column] = bc_ref[:, column]
            for k in range(1, 8):
                bc_copy(k, back=True).wait_recv()
            for half in range(2):
                summed = bc_in[0, half].astype(F32)
                for k in range(1, 8):
                    summed = summed + bc_in[k, half].astype(F32)
                bc_sum[half] = summed
            bc_half().start()

        @pl.when(t == 0)
        def _():
            from_source(0, 1 - core).wait_recv()
            each(0, 0, "start")

        @pl.when(jnp.logical_and(t >= 1, t < turns))
        def _():
            for c in range(2):
                from_source(t, c).wait_recv()
            each(t, 0, "start")

        @pl.when(jnp.logical_and(t >= 1, t < turns + 1))
        def _():
            each(t - 1, 0, "wait_recv")
            each(t - 1, 1, "start")

        @pl.when(jnp.logical_and(t >= 2, t < turns + 2))
        def _():
            each(t - 2, 1, "wait_recv")
            each(t - 2, 2, "start")

        @pl.when(t == 2)
        def _():
            load_w.wait()

        @pl.when(t >= 3)
        def _():
            each(t - 3, 2, "wait_recv")
            compute(t - 3)

        return carry

    shares[...] = jnp.zeros_like(shares)
    lax.fori_loop(0, turns + 3, pass_on, 0)
    all_exp = 16
    own = (chip_y * 4 + chip_z) * 2 + core

    def exp_device(index):
        return {"exp_0": lax.div(index, 8), "exp_1": lax.rem(lax.div(index, 2), 4), "exp_2": lax.rem(index, 2)}

    def part(k, back=False):
        to, source = lax.rem(seq + k, 8), lax.rem(seq + (8 - k), 8)
        return pltpu.make_async_remote_copy(
            src_ref=part_in.at[source] if back else part_out.at[to],
            dst_ref=part_in.at[source] if back else part_in.at[seq],
            send_sem=p_send.at[k - 1], recv_sem=p_recv.at[k - 1], device_id={"seq": to}, device_id_type=MESH,
        )

    def total(k, back=False):
        to, source = lax.rem(own + k, all_exp), lax.rem(own + (all_exp - k), all_exp)
        return pltpu.make_async_remote_copy(
            src_ref=sum_in.at[source] if back else sum_out.at[to],
            dst_ref=sum_in.at[source] if back else sum_in.at[own],
            send_sem=q_send.at[k - 1], recv_sem=q_recv.at[k - 1], device_id=exp_device(to), device_id_type=MESH,
        )

    for k in range(8):
        part_out[k] = shares[k : k + 1, :]
    for k in range(1, 8):
        part(k).start()
    part_in[seq] = part_out[seq]
    for k in range(1, 8):
        part(k, back=True).wait_recv()
    summed = part_in[0]
    for k in range(1, 8):
        summed = summed + part_in[k]
    at = lambda dim, *shape: lax.broadcasted_iota(jnp.int32, shape, dim)
    width = summed.shape[1]
    each_exp = jnp.where(lax.div(at(1, all_exp, width), slots) == at(0, all_exp, width), summed, 0.0)
    each_exp = exactly(each_exp, lax.rem(at(0, width, 128), slots) == at(1, width, 128))
    for k in range(all_exp):
        sum_out[k] = each_exp[k : k + 1, :]
    for k in range(1, all_exp):
        total(k).start()
    sum_in[own] = sum_out[own]
    for k in range(1, all_exp):
        total(k, back=True).wait_recv()
    for k in range(all_exp):
        route_ref[k : k + 1, :] = sum_in[k]
    for k in range(1, 8):
        part(k).wait_send()
    for k in range(1, all_exp):
        total(k).wait_send()
    bc_half().wait_recv()
    summed = bc_sum[chip_y] + bc_other[...]
    b_ref[...] = summed[:, :128]
    c_ref[...] = summed[:, 128:]
    bc_half().wait_send()
    for k in range(1, 8):
        bc_copy(k).wait_send()
    store_pre(turns - 2).wait()
    store_pre(turns - 1).wait()
    to_expert(0, 1 - core).wait_send()
    for turn in range(1, turns):
        for k in range(2):
            to_expert(turn, k).wait_send()

    def sent(i, carry):
        for step in range(3):
            each(i, step, "wait_send")
        return carry

    lax.fori_loop(0, turns, sent, 0)


def expert_part(keep, other, residual, select, slot_gates, bc_grads, w_down, saved_pre):
    slots, _, hidden = saved_pre.shape[1:]
    d = residual.shape[1]
    rows = select.shape[0]
    turns, block = 8, rows // 8
    vmem = pl.BlockSpec(memory_space=pltpu.VMEM)
    hbm = pl.BlockSpec(memory_space=pl.ANY)
    dma = pltpu.SemaphoreType.DMA
    tokens = residual.shape[0]
    bc_grads = bc_grads.reshape(2, 8, tokens, 256)
    pre, route, b_grads, c_grads = pl.pallas_call(
        expert_kernel,
        out_shape=(
            jax.ShapeDtypeStruct((8, turns, block, 2, hidden), BF16),
            jax.ShapeDtypeStruct((16, 128), F32),
            jax.ShapeDtypeStruct((tokens, 128), F32),
            jax.ShapeDtypeStruct((tokens, 128), F32),
        ),
        in_specs=[vmem] * 6 + [hbm] * 2,
        out_specs=(hbm, vmem, vmem, vmem),
        scratch_shapes=[
            pltpu.VMEM((16, rows // 16, d), BF16),
            pltpu.VMEM((turns, 2, 4, block, d), BF16),
            pltpu.VMEM((hidden, d), BF16),
            pltpu.VMEM((2, 8, block, 2, hidden), BF16),
            pltpu.VMEM((2, 8, block, 2, hidden), BF16),
            pltpu.VMEM((8, turns * block), F32),
            pltpu.VMEM((8, 1, turns * block), F32),
            pltpu.VMEM((8, 1, turns * block), F32),
            pltpu.VMEM((16, 1, 128), F32),
            pltpu.VMEM((16, 1, 128), F32),
            pltpu.VMEM((8, 2, tokens, 256), BF16),
            pltpu.VMEM((2, tokens, 256), F32),
            pltpu.VMEM((tokens, 256), F32),
            dma((1,)),
            dma((2,)),
            dma((2,)),
            dma((turns, 2)),
            dma((turns, 2)),
            dma((turns, 10)),
            dma((turns, 10)),
            dma((7,)),
            dma((7,)),
            dma((15,)),
            dma((15,)),
            dma((8,)),
            dma((8,)),
        ],
        compiler_params=pltpu.CompilerParams(
            collective_id=2, has_side_effects=True, vmem_limit_bytes=60 * 2**20
        ),
        name="experts",
    )(keep, other, residual, select, slot_gates, bc_grads, w_down, saved_pre.reshape(8, turns, block, 2, hidden))
    return pre.reshape(saved_pre.shape), route[:, : block // 2].reshape(-1), b_grads, c_grads


def per_device(
    gates, expert_ids, saved_pre, w_down, residual_grad, in_weight, ssm_in, b_proj, c_proj, step_sizes, a_log, skip_gain, ssm_grad
):
    w_all, x_all, bc_grads, step_grads = ssm_part(
        in_weight, ssm_in, b_proj, c_proj, step_sizes, a_log, skip_gain, ssm_grad
    )
    tokens_here = residual_grad.shape[0]
    experts = lax.axis_size(EXP)
    capacity = TOPK * tokens_here // experts
    keep, send = project(x_all, w_all)
    other = lax.ppermute(send, CORE, [(0, 1), (1, 0)])
    flat_ids = expert_ids.reshape(-1)
    onehot = (flat_ids[:, None] == jnp.arange(experts, dtype=jnp.int32)[None, :]).astype(jnp.int32)
    position = jnp.sum(onehot * jnp.cumsum(onehot, axis=0), axis=1) - 1
    target = flat_ids * capacity + position
    selector = target[:, None] == jnp.arange(experts * capacity, dtype=jnp.int32)[None, :]
    by_token = selector.reshape(tokens_here, TOPK, -1)
    slot_gates = jnp.sum(by_token * gates[:, :, None], axis=(0, 1))
    select = jnp.any(by_token, axis=1).astype(BF16).T
    pre_grads, totals, b_grads, c_grads = expert_part(
        keep, other, residual_grad, select, slot_gates[:, None], bc_grads, w_down, saved_pre
    )
    route_grads = totals[target].reshape(tokens_here, TOPK) / gates
    return (pre_grads, route_grads, b_grads, c_grads, step_grads)


def solution(mesh):
    split = Mesh(mesh.devices.reshape(mesh.shape["seq"], 2, 4, 2), ("seq", "exp_0", "exp_1", "exp_2"))
    in_specs = (
        P(SEQ_EXP, None), P(SEQ_EXP, None), P(EXP, None, None, "seq"), P(EXP, "seq", None), P(SEQ_EXP, None), P("seq", EXP),
        P("seq", EXP), P("seq", None), P("seq", None), P(EXP, "seq"), P(EXP), P(EXP), P("seq", EXP),
    )
    out_specs = (P(EXP, None, None, "seq"), P(SEQ_EXP, None), P(SEQ_EXP, None), P(SEQ_EXP, None), P(EXP, "seq"))
    return jax.shard_map(per_device, mesh=split, in_specs=in_specs, out_specs=out_specs, check_vma=False)
```
